128 devices in a mesh: lat: 4 (over z), lon: 4 (over x_lo, core), lev: 8 (over y, x_hi).
Axes of the slice: x: 4 (x_hi: 2, x_lo: 2; x = x_hi * 2 + x_lo), y: 4, z: 4, core: 2. Of those that a mesh axis runs over, the one named last changes fastest.
Arguments:
- field_now: float32 [16, 256, 512, 128], P('lat', 'lon', 'lev'), may hold values from 0.2 to 1.8
- earlier: float32 [16, 256, 512, 128], P('lat', 'lon', 'lev'), may hold values from 0.2 to 1.8
- speed_square: float32 [16, 256, 512, 128], P('lat', 'lon', 'lev'), may hold values from 0.05 to 0.3
Outputs:
- field_now_end: float32 [16, 256, 512, 128], P('lat', 'lon', 'lev')
The draws below stay inside these ranges and needn't reach their ends.
All inputs are finite; a program needn't handle non-finite values.
Results may differ from the reference program's by a relative error of at most 0.00002.
Values sent between devices are 32-bit elements; how exact they have to be, the bound alone decides.
A program may use at most 320 MiB of HBM per device.

```python
import jax
import jax.numpy as jnp
from jax import lax

GRID_J = 16
GRID_I = 256
GRID_K = 512
MEMBERS = 128
STEPS = 4


def block_levels(stream_key, shape, cuts, least, largest):
    def one(axis_at, blocks):
        draws = jax.random.uniform(jax.random.fold_in(jax.random.fold_in(stream_key, 6), axis_at), (blocks,), jnp.float32, least / len(cuts), largest / len(cuts))
        return jnp.repeat(jnp.exp(draws), shape[axis_at] // blocks).reshape((-1,) + (1,) * (len(shape) - axis_at - 1))

    gain = one(*cuts[0])
    for cut in cuts[1:]:
        gain = gain * one(*cut)
    return gain


def setup_inputs(seed: int = 0) -> dict:
    arg_keys = jax.random.split(jax.random.key(seed), 4)
    field_now = jnp.clip(0.2 + 1.5999999 * jax.random.uniform(arg_keys[0], (GRID_J, GRID_I, GRID_K, MEMBERS), jnp.float32) ** block_levels(arg_keys[0], (GRID_J, GRID_I, GRID_K, MEMBERS), ((0, 4), (1, 4), (2, 8)), -0.2, 0.2), 0.2, 1.8)
    earlier = jnp.clip(0.2 + 1.5999999 * jax.random.uniform(arg_keys[1], (GRID_J, GRID_I, GRID_K, MEMBERS), jnp.float32) ** block_levels(arg_keys[1], (GRID_J, GRID_I, GRID_K, MEMBERS), ((0, 4), (1, 4), (2, 8)), -0.2, 0.2), 0.2, 1.8)
    speed_square = jnp.clip(0.05 + 0.25 * jax.random.uniform(arg_keys[2], (GRID_J, GRID_I, GRID_K, MEMBERS), jnp.float32) ** block_levels(arg_keys[2], (GRID_J, GRID_I, GRID_K, MEMBERS), ((0, 4), (1, 4), (2, 8)), -0.2, 0.2), 0.05, 0.3)
    return {"field_now": field_now, "earlier": earlier, "speed_square": speed_square}


def without_rim(values, dims):
    for dim in dims:
        values = lax.slice_in_dim(values, 1, values.shape[dim] - 1, axis=dim)
    return values


def shifted_cells(values, dim, start, dims):
    others = [other for other in dims if other != dim]
    values = without_rim(values, others)
    return lax.slice_in_dim(values, start, start + values.shape[dim] - 2, axis=dim)


def march_step(padded, before, speed_square):
    middle = without_rim(padded, (0, 1, 2))
    lower = [shifted_cells(padded, dim, 0, (0, 1, 2)) for dim in (0, 1, 2)]
    upper = [shifted_cells(padded, dim, 2, (0, 1, 2)) for dim in (0, 1, 2)]
    spread = lower[0] + upper[0] + lower[1] + upper[1] + lower[2] + upper[2] - 6.0 * middle
    return 2.0 * middle - before + speed_square * spread


def reference(field_now, earlier, speed_square):
    for step in range(STEPS):
        later = march_step(jnp.pad(field_now, ((1, 1), (1, 1), (1, 1), (0, 0)), mode="constant"), earlier, speed_square)
        earlier, field_now = field_now, later
    return field_now
```

```python
import functools

import jax
import jax.numpy as jnp
from jax import lax
from jax.experimental import pallas as pl
from jax.experimental.pallas import tpu as pltpu
from jax.sharding import PartitionSpec as P

STEPS = 4
CHUNK = 8
MESH = pl.DeviceIdType.MESH


def kernel(
    now_ref, earlier_ref, speed_ref, out_ref,
    field, speed, halo_j, halo_k, pack_k,
    load_sem, out_sem, send_j, recv_j, send_i, recv_i, send_k, recv_k,
):
    planes, rows, depth, _ = now_ref.shape
    chunks = rows // CHUNK
    place = [lax.axis_index(axis) for axis in ("lat", "lon", "lev")]
    sizes = [lax.axis_size(axis) for axis in ("lat", "lon", "lev")]
    has = [(at > 0, at < size - 1) for at, size in zip(place, sizes)]
    towards = [
        tuple({axis: at + shift} for shift in (-1, 1))
        for axis, at in zip(("lat", "lon", "lev"), place)
    ]

    loads = [
        pltpu.make_async_copy(now_ref, field.at[0, :, pl.ds(1, rows)], load_sem.at[0]),
        pltpu.make_async_copy(earlier_ref, field.at[1, :, pl.ds(1, rows)], load_sem.at[1]),
        pltpu.make_async_copy(speed_ref, speed, load_sem.at[2]),
    ]
    for load in loads:
        load.start()

    barrier = pltpu.get_barrier_semaphore()
    count = 0
    for axis in range(3):
        for side in range(2):
            count = count + has[axis][side].astype(jnp.int32)

            @pl.when(has[axis][side])
            def _():
                pl.semaphore_signal(barrier, inc=1, device_id=towards[axis][side], device_id_type=MESH)

    pl.semaphore_wait(barrier, count)

    def copy_j(step, chunk, side):
        plane = (planes - 1) * side
        at = pl.multiple_of(chunk * CHUNK, CHUNK)
        if step == 0:
            source = now_ref.at[plane, pl.ds(at, CHUNK)]
        else:
            source = field.at[step % 2, plane, pl.ds(at + 1, CHUNK)]
        return pltpu.make_async_remote_copy(
            src_ref=source,
            dst_ref=halo_j.at[step, 1 - side, pl.ds(at, CHUNK)],
            send_sem=send_j.at[step, side, chunk],
            recv_sem=recv_j.at[step, 1 - side, chunk],
            device_id=towards[0][side],
            device_id_type=MESH,
        )

    def wait_j(step, chunk, side):
        at = pl.multiple_of(chunk * CHUNK, CHUNK)
        piece = halo_j.at[step, side, pl.ds(at, CHUNK)]
        pltpu.make_async_remote_copy(
            src_ref=piece, dst_ref=piece,
            send_sem=send_j.at[step, 1 - side, chunk],
            recv_sem=recv_j.at[step, side, chunk],
            device_id=towards[0][side], device_id_type=MESH,
        ).wait_recv()

    def copy_i(step, side):
        return pltpu.make_async_remote_copy(
            src_ref=field.at[step % 2, :, 1 + (rows - 1) * side],
            dst_ref=field.at[step % 2, :, (rows + 1) * (1 - side)],
            send_sem=send_i.at[step, side],
            recv_sem=recv_i.at[step, 1 - side],
            device_id=towards[1][side],
            device_id_type=MESH,
        )

    def copy_k(step, side):
        return pltpu.make_async_remote_copy(
            src_ref=pack_k.at[step, side],
            dst_ref=halo_k.at[step, 1 - side],
            send_sem=send_k.at[step, side],
            recv_sem=recv_k.at[step, 1 - side],
            device_id=towards[2][side],
            device_id_type=MESH,
        )

    def pack(step):
        def row(i, _):
            for plane in range(planes):
                for side in range(2):
                    pack_k[step, side, plane, pl.ds(i, 1), :] = field[step % 2, plane, i + 1, pl.ds((depth - 1) * side, 1), :]
            return 0

        lax.fori_loop(0, rows, row, 0)

    def send_sides(step):
        for side in range(2):
            @pl.when(has[1][side])
            def _():
                copy_i(step, side).start()

        for side in range(2):
            @pl.when(has[2][side])
            def _():
                copy_k(step, side).start()

    def wait_sides(step):
        for side in range(2):
            @pl.when(has[1][1 - side])
            def _():
                copy_i(step, side).wait_recv()

            @pl.when(has[2][1 - side])
            def _():
                copy_k(step, side).wait_recv()

    def wait_sides_sent(step):
        for side in range(2):
            @pl.when(has[1][side])
            def _():
                copy_i(step, side).wait_send()

            @pl.when(has[2][side])
            def _():
                copy_k(step, side).wait_send()

    def send_chunk(step, chunk):
        for side in range(2):
            @pl.when(has[0][side])
            def _():
                copy_j(step, chunk, side).start()

    def wait_chunk_sent(step, chunk):
        for side in range(2):
            @pl.when(has[0][side])
            def _():
                copy_j(step, chunk, side).wait_send()

    def each_chunk(body):
        def one(chunk, _):
            body(chunk)
            return 0

        lax.fori_loop(0, chunks, one, 0)

    each_chunk(lambda chunk: send_chunk(0, chunk))

    for side in range(2):
        @pl.when(jnp.logical_not(has[1][side]))
        def _():
            for slot in range(2):
                field[slot, :, (rows + 1) * side] = jnp.zeros((planes, depth, 128), jnp.float32)

        @pl.when(jnp.logical_not(has[2][side]))
        def _():
            for step in range(STEPS):
                for plane in range(planes):
                    halo_k[step, side, plane] = jnp.zeros((rows, 128), jnp.float32)

        @pl.when(jnp.logical_not(has[0][side]))
        def _():
            def row(i, _):
                halo_j[0, side, i] = jnp.zeros((depth, 128), jnp.float32)
                return 0

            lax.fori_loop(0, rows, row, 0)

    loads[0].wait()
    pack(0)
    send_sides(0)
    loads[1].wait()
    loads[2].wait()

    level = lax.broadcasted_iota(jnp.int32, (depth, 128), 0)
    first, last = level == 0, level == depth - 1

    def compute_row(step, i):
        old, new = step % 2, (step + 1) % 2
        slots = [jnp.where(has[0][side], step, 0) for side in range(2)]
        for plane in range(planes):
            here = field[old, plane, i + 1]
            below = halo_j[slots[0], 0, i] if plane == 0 else field[old, plane - 1, i + 1]
            above = halo_j[slots[1], 1, i] if plane == planes - 1 else field[old, plane + 1, i + 1]
            spread = below + above + field[old, plane, i] + field[old, plane, i + 2]
            k_low = jnp.where(first, halo_k[step, 0, plane, pl.ds(i, 1), :], pltpu.roll(here, 1, 0))
            k_high = jnp.where(last, halo_k[step, 1, plane, pl.ds(i, 1), :], pltpu.roll(here, depth - 1, 0))
            spread = spread + k_low + k_high - 6.0 * here
            field[new, plane, i + 1] = 2.0 * here - field[new, plane, i + 1] + speed[plane, i] * spread

    def copy_out(chunk):
        at = pl.multiple_of(chunk * CHUNK, CHUNK)
        return pltpu.make_async_copy(
            field.at[STEPS % 2, :, pl.ds(at + 1, CHUNK)], out_ref.at[:, pl.ds(at, CHUNK)], out_sem.at[chunk]
        )

    for step in range(STEPS):
        wait_sides(step)
        if step > 0:
            wait_sides_sent(step - 1)

        def one_chunk(chunk):
            if step > 0:
                wait_chunk_sent(step - 1, chunk)
            for side in range(2):
                @pl.when(has[0][side])
                def _():
                    wait_j(step, chunk, side)

            def row(i, _):
                compute_row(step, chunk * CHUNK + i)
                return 0

            lax.fori_loop(0, CHUNK, row, 0)
            if step < STEPS - 1:
                @pl.when(chunk > 0)
                def _():
                    send_chunk(step + 1, chunk - 1)
            else:
                copy_out(chunk).start()

        each_chunk(one_chunk)
        if step < STEPS - 1:
            pack(step + 1)
            send_chunk(step + 1, chunks - 1)
            send_sides(step + 1)

    wait_sides_sent(STEPS - 1)
    each_chunk(lambda chunk: wait_chunk_sent(STEPS - 1, chunk))
    each_chunk(lambda chunk: copy_out(chunk).wait())


def local(field_now, earlier, speed_square):
    planes, rows, depth, members = field_now.shape
    chunks = rows // CHUNK
    f32 = jnp.float32
    any_spec = pl.BlockSpec(memory_space=pl.ANY)
    return pl.pallas_call(
        kernel,
        out_shape=jax.ShapeDtypeStruct(field_now.shape, f32),
        in_specs=[any_spec] * 3,
        out_specs=any_spec,
        scratch_shapes=[
            pltpu.VMEM((2, planes, rows + 2, depth, members), f32),
            pltpu.VMEM((planes, rows, depth, members), f32),
            pltpu.VMEM((STEPS, 2, rows, depth, members), f32),
            pltpu.VMEM((STEPS, 2, planes, rows, members), f32),
            pltpu.VMEM((STEPS, 2, planes, rows, members), f32),
            pltpu.SemaphoreType.DMA((3,)),
            pltpu.SemaphoreType.DMA((chunks,)),
            pltpu.SemaphoreType.DMA((STEPS, 2, chunks)),
            pltpu.SemaphoreType.DMA((STEPS, 2, chunks)),
            pltpu.SemaphoreType.DMA((STEPS, 2)),
            pltpu.SemaphoreType.DMA((STEPS, 2)),
            pltpu.SemaphoreType.DMA((STEPS, 2)),
            pltpu.SemaphoreType.DMA((STEPS, 2)),
        ],
        compiler_params=pltpu.CompilerParams(
            collective_id=0, has_side_effects=True, vmem_limit_bytes=60 * 2**20
        ),
    )(field_now, earlier, speed_square)


def solution(mesh):
    spec = P("lat", "lon", "lev", None)
    return jax.shard_map(local, mesh=mesh, in_specs=(spec,) * 3, out_specs=spec, check_vma=False)
```

```python
import functools

import jax
import jax.numpy as jnp
from jax import lax
from jax.experimental import pallas as pl
from jax.experimental.pallas import tpu as pltpu
from jax.sharding import PartitionSpec as P

STEPS = 4
CHUNK = 8
PIECE = (8, 8, 8, 4)
MESH = pl.DeviceIdType.MESH


def kernel(
    now_ref, earlier_ref, speed_ref, out_ref,
    field, speed, halo_j, halo_k, pack_k,
    load_sem, send_j, recv_j, send_i, recv_i, send_k, recv_k,
):
    planes, rows, depth, _ = now_ref.shape
    chunks = rows // CHUNK
    place = [lax.axis_index(axis) for axis in ("lat", "lon", "lev")]
    sizes = [lax.axis_size(axis) for axis in ("lat", "lon", "lev")]
    has = [(at > 0, at < size - 1) for at, size in zip(place, sizes)]
    towards = [
        tuple({axis: at + shift} for shift in (-1, 1))
        for axis, at in zip(("lat", "lon", "lev"), place)
    ]

    spans = [(plane, 1, at, size) for at, size in ((0, CHUNK), (CHUNK, rows - CHUNK)) for plane in (0, planes - 1)]
    spans.append((1, planes - 2, 0, rows))
    loads = [
        pltpu.make_async_copy(
            now_ref.at[pl.ds(plane, count), pl.ds(at, size)],
            field.at[0, pl.ds(plane, count), pl.ds(at + 1, size)],
            load_sem.at[index],
        )
        for index, (plane, count, at, size) in enumerate(spans)
    ]
    loads.append(pltpu.make_async_copy(earlier_ref, field.at[1, :, pl.ds(1, rows)], load_sem.at[5]))
    loads.append(pltpu.make_async_copy(speed_ref, speed, load_sem.at[6]))
    for load in loads:
        load.start()

    barrier = pltpu.get_barrier_semaphore()
    count = 0
    for axis in range(3):
        for side in range(2):
            count = count + has[axis][side].astype(jnp.int32)

            @pl.when(has[axis][side])
            def _():
                pl.semaphore_signal(barrier, inc=1, device_id=towards[axis][side], device_id_type=MESH)

    pl.semaphore_wait(barrier, count)

    def copy_j(step, piece, side):
        at = pl.multiple_of(piece * PIECE[step], PIECE[step])
        return pltpu.make_async_remote_copy(
            src_ref=field.at[step % 2, (planes - 1) * side, pl.ds(at + 1, PIECE[step])],
            dst_ref=halo_j.at[step, 1 - side, pl.ds(at, PIECE[step])],
            send_sem=send_j.at[step, side, piece],
            recv_sem=recv_j.at[step, 1 - side, piece],
            device_id=towards[0][side],
            device_id_type=MESH,
        )

    def copy_i(step, side):
        return pltpu.make_async_remote_copy(
            src_ref=field.at[step % 2, :, 1 + (rows - 1) * side],
            dst_ref=field.at[step % 2, :, (rows + 1) * (1 - side)],
            send_sem=send_i.at[step, side],
            recv_sem=recv_i.at[step, 1 - side],
            device_id=towards[1][side],
            device_id_type=MESH,
        )

    def copy_k(step, side):
        return pltpu.make_async_remote_copy(
            src_ref=pack_k.at[step, side],
            dst_ref=halo_k.at[step, 1 - side],
            send_sem=send_k.at[step, side],
            recv_sem=recv_k.at[step, 1 - side],
            device_id=towards[2][side],
            device_id_type=MESH,
        )

    def pack(step):
        def row(i, _):
            for plane in range(planes):
                for side in range(2):
                    pack_k[step, side, plane, pl.ds(i, 1), :] = field[step % 2, plane, i + 1, pl.ds((depth - 1) * side, 1), :]
            return 0

        lax.fori_loop(0, rows, row, 0)

    def send_sides(step):
        for side in range(2):
            @pl.when(has[1][side])
            def _():
                copy_i(step, side).start()

        for side in range(2):
            @pl.when(has[2][side])
            def _():
                copy_k(step, side).start()

    def wait_sides(step):
        for side in range(2):
            @pl.when(has[1][1 - side])
            def _():
                copy_i(step, side).wait_recv()

            @pl.when(has[2][1 - side])
            def _():
                copy_k(step, side).wait_recv()

    def wait_sides_sent(step):
        for side in range(2):
            @pl.when(has[1][side])
            def _():
                copy_i(step, side).wait_send()

            @pl.when(has[2][side])
            def _():
                copy_k(step, side).wait_send()

    def send_piece(step, piece):
        for side in range(2):
            @pl.when(has[0][side])
            def _():
                copy_j(step, piece, side).start()

    def wait_piece_sent(step, piece):
        for side in range(2):
            @pl.when(has[0][side])
            def _():
                copy_j(step, piece, side).wait_send()

    def wait_piece(step, piece):
        for side in range(2):
            @pl.when(has[0][1 - side])
            def _():
                copy_j(step, piece, side).wait_recv()

    def each(count, body):
        def one(index, _):
            body(index)
            return 0

        lax.fori_loop(0, count, one, 0)

    def send_chunk(step, chunk):
        pieces = CHUNK // PIECE[step]
        for index in range(pieces):
            send_piece(step, chunk * pieces + index)

    loads[0].wait()
    loads[1].wait()
    send_chunk(0, 0)
    loads[2].wait()
    loads[3].wait()
    each(chunks - 1, lambda chunk: send_chunk(0, chunk + 1))

    for side in range(2):
        @pl.when(jnp.logical_not(has[1][side]))
        def _():
            for slot in range(2):
                field[slot, :, (rows + 1) * side] = jnp.zeros((planes, depth, 128), jnp.float32)

        @pl.when(jnp.logical_not(has[2][side]))
        def _():
            for step in range(STEPS):
                for plane in range(planes):
                    halo_k[step, side, plane] = jnp.zeros((rows, 128), jnp.float32)

        @pl.when(jnp.logical_not(has[0][side]))
        def _():
            def row(i, _):
                halo_j[0, side, i] = jnp.zeros((depth, 128), jnp.float32)
                return 0

            lax.fori_loop(0, rows, row, 0)

    loads[4].wait()
    pack(0)
    send_sides(0)
    loads[5].wait()
    loads[6].wait()

    level = lax.broadcasted_iota(jnp.int32, (depth, 128), 0)
    first, last = level == 0, level == depth - 1

    def compute_row(step, i, some):
        old, new = step % 2, (step + 1) % 2
        slots = [jnp.where(has[0][side], step, 0) for side in range(2)]
        for plane in some:
            here = field[old, plane, i + 1]
            below = halo_j[slots[0], 0, i] if plane == 0 else field[old, plane - 1, i + 1]
            above = halo_j[slots[1], 1, i] if plane == planes - 1 else field[old, plane + 1, i + 1]
            spread = below + above + field[old, plane, i] + field[old, plane, i + 2]
            k_low = jnp.where(first, halo_k[step, 0, plane, pl.ds(i, 1), :], pltpu.roll(here, 1, 0))
            k_high = jnp.where(last, halo_k[step, 1, plane, pl.ds(i, 1), :], pltpu.roll(here, depth - 1, 0))
            spread = spread + k_low + k_high - 6.0 * here
            later = 2.0 * here - field[new, plane, i + 1] + speed[plane, i] * spread
            if step < STEPS - 1:
                field[new, plane, i + 1] = later
            else:
                out_ref[plane, i] = later

    def compute(step, at, size, some):
        each(size, lambda i: compute_row(step, at + i, some))

    for step in range(STEPS - 1):
        wait_sides(step)
        if step > 0:
            wait_sides_sent(step - 1)

        def one_chunk(chunk):
            if step > 0:
                wait_piece_sent(step - 1, chunk)
            wait_piece(step, chunk)
            compute(step, chunk * CHUNK, CHUNK, range(planes))

            @pl.when(chunk > 0)
            def _():
                send_chunk(step + 1, chunk - 1)

        each(chunks, one_chunk)
        pack(step + 1)
        send_chunk(step + 1, chunks - 1)
        send_sides(step + 1)

    last_step, size = STEPS - 1, PIECE[STEPS - 1]
    wait_sides(last_step)
    wait_sides_sent(last_step - 1)

    def one_piece(piece):
        compute(last_step, piece * size, size, range(1, planes - 1))
        wait_piece(last_step, piece)
        compute(last_step, piece * size, size, (0, planes - 1))

    each(rows // size, one_piece)
    each(chunks, lambda chunk: wait_piece_sent(last_step - 1, chunk))
    each(rows // size, lambda piece: wait_piece_sent(last_step, piece))
    wait_sides_sent(last_step)


def write_out(value_ref, out_ref, sem):
    rows = value_ref.shape[1]
    copies = [
        pltpu.make_async_copy(value_ref.at[:, pl.ds(at, CHUNK)], out_ref.at[:, pl.ds(at, CHUNK)], sem.at[at // CHUNK])
        for at in range(0, rows, CHUNK)
    ]
    for copy in copies:
        copy.start()
    for copy in copies:
        copy.wait()


def local(field_now, earlier, speed_square):
    planes, rows, depth, members = field_now.shape
    f32 = jnp.float32
    any_spec = pl.BlockSpec(memory_space=pl.ANY)
    later = pl.pallas_call(
        kernel,
        out_shape=pltpu.VMEM(field_now.shape, f32),
        in_specs=[any_spec] * 3,
        out_specs=pl.BlockSpec(memory_space=pltpu.VMEM),
        scratch_shapes=[
            pltpu.VMEM((2, planes, rows + 2, depth, members), f32),
            pltpu.VMEM((planes, rows, depth, members), f32),
            pltpu.VMEM((STEPS, 2, rows, depth, members), f32),
            pltpu.VMEM((STEPS, 2, planes, rows, members), f32),
            pltpu.VMEM((STEPS, 2, planes, rows, members), f32),
            pltpu.SemaphoreType.DMA((7,)),
            pltpu.SemaphoreType.DMA((STEPS, 2, rows // min(PIECE))),
            pltpu.SemaphoreType.DMA((STEPS, 2, rows // min(PIECE))),
            pltpu.SemaphoreType.DMA((STEPS, 2)),
            pltpu.SemaphoreType.DMA((STEPS, 2)),
            pltpu.SemaphoreType.DMA((STEPS, 2)),
            pltpu.SemaphoreType.DMA((STEPS, 2)),
        ],
        compiler_params=pltpu.CompilerParams(
            collective_id=0, has_side_effects=True, vmem_limit_bytes=46 * 2**20
        ),
    )(field_now, earlier, speed_square)
    return pl.pallas_call(
        write_out,
        out_shape=jax.ShapeDtypeStruct(field_now.shape, f32),
        in_specs=[pl.BlockSpec(memory_space=pltpu.VMEM)],
        out_specs=any_spec,
        scratch_shapes=[pltpu.SemaphoreType.DMA((rows // CHUNK,))],
        compiler_params=pltpu.CompilerParams(vmem_limit_bytes=2**20),
    )(later)


def solution(mesh):
    spec = P("lat", "lon", "lev", None)
    return jax.shard_map(local, mesh=mesh, in_specs=(spec,) * 3, out_specs=spec, check_vma=False)
```

```python
import functools

import jax
import jax.numpy as jnp
from jax import lax
from jax.experimental import pallas as pl
from jax.experimental.pallas import tpu as pltpu
from jax.sharding import PartitionSpec as P

STEPS = 4
PIECES = ((32, 32), (32, 32), (32, 32), (32, 24, 8))
OUT = 8
MESH = pl.DeviceIdType.MESH


def cuts(step, rows):
    sizes = [size * rows // sum(PIECES[step]) for size in PIECES[step]]
    return [(sum(sizes[:index]), size) for index, size in enumerate(sizes)]


def kernel(
    now_ref, earlier_ref, speed_ref, out_ref,
    field, speed, halo_j, halo_k, pack_k,
    load_sem, send_j, recv_j, send_i, recv_i, send_k, recv_k,
):
    planes, rows, depth, _ = now_ref.shape
    pieces = [cuts(step, rows) for step in range(STEPS)]
    place = [lax.axis_index(axis) for axis in ("lat", "lon", "lev")]
    sizes = [lax.axis_size(axis) for axis in ("lat", "lon", "lev")]
    has = [(at > 0, at < size - 1) for at, size in zip(place, sizes)]
    towards = [
        tuple({axis: at + shift} for shift in (-1, 1))
        for axis, at in zip(("lat", "lon", "lev"), place)
    ]

    spans = [(plane, 1, at, size) for at, size in pieces[0] for plane in (0, planes - 1)]
    spans.append((1, planes - 2, 0, rows))
    loads = [
        pltpu.make_async_copy(
            now_ref.at[pl.ds(plane, count), pl.ds(at, size)],
            field.at[0, pl.ds(plane, count), pl.ds(at + 1, size)],
            load_sem.at[index],
        )
        for index, (plane, count, at, size) in enumerate(spans)
    ]
    loads.append(pltpu.make_async_copy(earlier_ref, field.at[1, :, pl.ds(1, rows)], load_sem.at[5]))
    loads.append(pltpu.make_async_copy(speed_ref, speed, load_sem.at[6]))
    for load in loads:
        load.start()

    barrier = pltpu.get_barrier_semaphore()
    count = 0
    for axis in range(3):
        for side in range(2):
            count = count + has[axis][side].astype(jnp.int32)

            @pl.when(has[axis][side])
            def _():
                pl.semaphore_signal(barrier, inc=1, device_id=towards[axis][side], device_id_type=MESH)

    pl.semaphore_wait(barrier, count)

    def copy_j(step, piece, side):
        at, size = pieces[step][piece]
        return pltpu.make_async_remote_copy(
            src_ref=field.at[step % 2, (planes - 1) * side, pl.ds(at + 1, size)],
            dst_ref=halo_j.at[step, 1 - side, pl.ds(at, size)],
            send_sem=send_j.at[step, side, piece],
            recv_sem=recv_j.at[step, 1 - side, piece],
            device_id=towards[0][side],
            device_id_type=MESH,
        )

    def copy_i(step, side):
        return pltpu.make_async_remote_copy(
            src_ref=field.at[step % 2, :, 1 + (rows - 1) * side],
            dst_ref=field.at[step % 2, :, (rows + 1) * (1 - side)],
            send_sem=send_i.at[step, side],
            recv_sem=recv_i.at[step, 1 - side],
            device_id=towards[1][side],
            device_id_type=MESH,
        )

    def copy_k(step, side):
        return pltpu.make_async_remote_copy(
            src_ref=pack_k.at[step, side],
            dst_ref=halo_k.at[step, 1 - side],
            send_sem=send_k.at[step, side],
            recv_sem=recv_k.at[step, 1 - side],
            device_id=towards[2][side],
            device_id_type=MESH,
        )

    def pack(step):
        def row(i, _):
            for plane in range(planes):
                for side in range(2):
                    pack_k[step, side, plane, pl.ds(i, 1), :] = field[step % 2, plane, i + 1, pl.ds((depth - 1) * side, 1), :]
            return 0

        lax.fori_loop(0, rows, row, 0)

    def send_sides(step):
        for side in range(2):
            @pl.when(has[1][side])
            def _():
                copy_i(step, side).start()

        for side in range(2):
            @pl.when(has[2][side])
            def _():
                copy_k(step, side).start()

    def wait_sides(step):
        for side in range(2):
            @pl.when(has[1][1 - side])
            def _():
                copy_i(step, side).wait_recv()

            @pl.when(has[2][1 - side])
            def _():
                copy_k(step, side).wait_recv()

    def wait_sides_sent(step):
        for side in range(2):
            @pl.when(has[1][side])
            def _():
                copy_i(step, side).wait_send()

            @pl.when(has[2][side])
            def _():
                copy_k(step, side).wait_send()

    def send_piece(step, piece):
        for side in range(2):
            @pl.when(has[0][side])
            def _():
                copy_j(step, piece, side).start()

    def wait_piece_sent(step, piece):
        for side in range(2):
            @pl.when(has[0][side])
            def _():
                copy_j(step, piece, side).wait_send()

    def wait_piece(step, piece):
        for side in range(2):
            @pl.when(has[0][1 - side])
            def _():
                copy_j(step, piece, side).wait_recv()

    def each(count, body):
        def one(index, _):
            body(index)
            return 0

        lax.fori_loop(0, count, one, 0)

    for piece in range(len(pieces[0])):
        loads[2 * piece].wait()
        loads[2 * piece + 1].wait()
        send_piece(0, piece)

    for side in range(2):
        @pl.when(jnp.logical_not(has[1][side]))
        def _():
            for slot in range(2):
                field[slot, :, (rows + 1) * side] = jnp.zeros((planes, depth, 128), jnp.float32)

        @pl.when(jnp.logical_not(has[2][side]))
        def _():
            for step in range(STEPS):
                for plane in range(planes):
                    halo_k[step, side, plane] = jnp.zeros((rows, 128), jnp.float32)

        @pl.when(jnp.logical_not(has[0][side]))
        def _():
            def row(i, _):
                halo_j[0, side, i] = jnp.zeros((depth, 128), jnp.float32)
                return 0

            lax.fori_loop(0, rows, row, 0)

    loads[4].wait()
    pack(0)
    send_sides(0)
    loads[5].wait()
    loads[6].wait()

    level = lax.broadcasted_iota(jnp.int32, (depth, 128), 0)
    first, last = level == 0, level == depth - 1

    def compute_row(step, i, some):
        old, new = step % 2, (step + 1) % 2
        slots = [jnp.where(has[0][side], step, 0) for side in range(2)]
        for plane in some:
            here = field[old, plane, i + 1]
            below = halo_j[slots[0], 0, i] if plane == 0 else field[old, plane - 1, i + 1]
            above = halo_j[slots[1], 1, i] if plane == planes - 1 else field[old, plane + 1, i + 1]
            spread = below + above + field[old, plane, i] + field[old, plane, i + 2]
            k_low = jnp.where(first, halo_k[step, 0, plane, pl.ds(i, 1), :], pltpu.roll(here, 1, 0))
            k_high = jnp.where(last, halo_k[step, 1, plane, pl.ds(i, 1), :], pltpu.roll(here, depth - 1, 0))
            spread = spread + k_low + k_high - 6.0 * here
            later = 2.0 * here - field[new, plane, i + 1] + speed[plane, i] * spread
            if step < STEPS - 1:
                field[new, plane, i + 1] = later
            else:
                out_ref[plane, i] = later

    def compute(step, at, size, some):
        each(size, lambda i: compute_row(step, at + i, some))

    for step in range(STEPS - 1):
        wait_sides(step)
        if step > 0:
            wait_sides_sent(step - 1)
        sent = 0
        for piece, (at, size) in enumerate(pieces[step]):
            if step > 0:
                wait_piece_sent(step - 1, piece)
            wait_piece(step, piece)
            compute(step, at, size, range(planes))
            while sent < len(pieces[step + 1]) and sum(pieces[step + 1][sent]) <= at + size:
                send_piece(step + 1, sent)
                sent += 1
        pack(step + 1)
        send_sides(step + 1)

    step = STEPS - 1
    wait_sides(step)
    compute(step, 0, rows, range(1, planes - 1))
    for piece, (at, size) in enumerate(pieces[step]):
        wait_piece(step, piece)
        compute(step, at, size, (0, planes - 1))
    for before in (step - 1, step):
        wait_sides_sent(before)
        for piece in range(len(pieces[before])):
            wait_piece_sent(before, piece)


def write_out(value_ref, out_ref, sem):
    rows = value_ref.shape[1]
    copies = [
        pltpu.make_async_copy(value_ref.at[:, pl.ds(at, OUT)], out_ref.at[:, pl.ds(at, OUT)], sem.at[at // OUT])
        for at in range(0, rows, OUT)
    ]
    for copy in copies:
        copy.start()
    for copy in copies:
        copy.wait()


def local(field_now, earlier, speed_square):
    planes, rows, depth, members = field_now.shape
    f32 = jnp.float32
    any_spec = pl.BlockSpec(memory_space=pl.ANY)
    later = pl.pallas_call(
        kernel,
        out_shape=pltpu.VMEM(field_now.shape, f32),
        in_specs=[any_spec] * 3,
        out_specs=pl.BlockSpec(memory_space=pltpu.VMEM),
        scratch_shapes=[
            pltpu.VMEM((2, planes, rows + 2, depth, members), f32),
            pltpu.VMEM((planes, rows, depth, members), f32),
            pltpu.VMEM((STEPS, 2, rows, depth, members), f32),
            pltpu.VMEM((STEPS, 2, planes, rows, members), f32),
            pltpu.VMEM((STEPS, 2, planes, rows, members), f32),
            pltpu.SemaphoreType.DMA((7,)),
            pltpu.SemaphoreType.DMA((STEPS, 2, max(map(len, PIECES)))),
            pltpu.SemaphoreType.DMA((STEPS, 2, max(map(len, PIECES)))),
            pltpu.SemaphoreType.DMA((STEPS, 2)),
            pltpu.SemaphoreType.DMA((STEPS, 2)),
            pltpu.SemaphoreType.DMA((STEPS, 2)),
            pltpu.SemaphoreType.DMA((STEPS, 2)),
        ],
        compiler_params=pltpu.CompilerParams(
            collective_id=0, has_side_effects=True, vmem_limit_bytes=46 * 2**20
        ),
    )(field_now, earlier, speed_square)
    return pl.pallas_call(
        write_out,
        out_shape=jax.ShapeDtypeStruct(field_now.shape, f32),
        in_specs=[pl.BlockSpec(memory_space=pltpu.VMEM)],
        out_specs=any_spec,
        scratch_shapes=[pltpu.SemaphoreType.DMA((rows // OUT,))],
        compiler_params=pltpu.CompilerParams(vmem_limit_bytes=2**20),
    )(later)


def solution(mesh):
    spec = P("lat", "lon", "lev", None)
    return jax.shard_map(local, mesh=mesh, in_specs=(spec,) * 3, out_specs=spec, check_vma=False)
```

```python
import functools

import jax
import jax.numpy as jnp
from jax import lax
from jax.experimental import pallas as pl
from jax.experimental.pallas import tpu as pltpu
from jax.sharding import PartitionSpec as P

STEPS = 4
PIECES = ((32, 32), (32, 32), (32, 32), (28, 30, 6))
EARLY = (1, 2)
MESH = pl.DeviceIdType.MESH


def cuts(step, rows):
    sizes = [size * rows // sum(PIECES[step]) for size in PIECES[step]]
    return [(sum(sizes[:index]), size) for index, size in enumerate(sizes)]


def kernel(
    now_ref, earlier_ref, speed_ref, inner_ref, outer_ref, face_ref, face_speed_ref, field, speed, halo_j, halo_k, pack_k,
    load_sem, send_j, recv_j, send_i, recv_i, send_k, recv_k,
):
    planes, rows, depth, _ = now_ref.shape
    pieces = [cuts(step, rows) for step in range(STEPS)]
    begin = pieces[-1][min(EARLY)][0]
    place = [lax.axis_index(axis) for axis in ("lat", "lon", "lev")]
    sizes = [lax.axis_size(axis) for axis in ("lat", "lon", "lev")]
    has = [(at > 0, at < size - 1) for at, size in zip(place, sizes)]
    towards = [
        tuple({axis: at + shift} for shift in (-1, 1))
        for axis, at in zip(("lat", "lon", "lev"), place)
    ]

    barrier = pltpu.get_barrier_semaphore()
    count = 0
    for axis in (2, 1, 0):
        for side in range(2):
            count = count + has[axis][side].astype(jnp.int32)

            @pl.when(has[axis][side])
            def _():
                pl.semaphore_signal(barrier, inc=1, device_id=towards[axis][side], device_id_type=MESH)

    spans = [(plane, 1, at, size) for at, size in pieces[0] for plane in (0, planes - 1)]
    spans.append((1, planes - 2, 0, rows))
    loads = [
        pltpu.make_async_copy(
            now_ref.at[pl.ds(plane, count), pl.ds(at, size)],
            field.at[0, pl.ds(plane, count), pl.ds(at + 1, size)],
            load_sem.at[index],
        )
        for index, (plane, count, at, size) in enumerate(spans)
    ]
    loads.append(pltpu.make_async_copy(earlier_ref, field.at[1, :, pl.ds(1, rows)], load_sem.at[5]))
    loads.append(pltpu.make_async_copy(speed_ref, speed, load_sem.at[6]))
    loads += [
        pltpu.make_async_copy(
            speed_ref.at[(planes - 1) * side, pl.ds(begin, rows - begin)], face_speed_ref.at[side], load_sem.at[7 + side]
        )
        for side in range(2)
    ]
    for load in loads:
        load.start()

    pl.semaphore_wait(barrier, count)

    def copy_j(step, piece, side):
        at, size = pieces[step][piece]
        if step == STEPS - 1 and at >= begin:
            source = face_ref.at[side, pl.ds(at - begin, size)]
        else:
            source = field.at[step % 2, (planes - 1) * side, pl.ds(at + 1, size)]
        return pltpu.make_async_remote_copy(
            src_ref=source,
            dst_ref=halo_j.at[step, 1 - side, pl.ds(at, size)],
            send_sem=send_j.at[step, side, piece],
            recv_sem=recv_j.at[step, 1 - side, piece],
            device_id=towards[0][side],
            device_id_type=MESH,
        )

    def copy_i(step, side):
        return pltpu.make_async_remote_copy(
            src_ref=field.at[step % 2, :, 1 + (rows - 1) * side],
            dst_ref=field.at[step % 2, :, (rows + 1) * (1 - side)],
            send_sem=send_i.at[step, side],
            recv_sem=recv_i.at[step, 1 - side],
            device_id=towards[1][side],
            device_id_type=MESH,
        )

    def copy_k(step, side):
        return pltpu.make_async_remote_copy(
            src_ref=pack_k.at[step, side],
            dst_ref=halo_k.at[step, 1 - side],
            send_sem=send_k.at[step, side],
            recv_sem=recv_k.at[step, 1 - side],
            device_id=towards[2][side],
            device_id_type=MESH,
        )

    def pack(step):
        def row(i, _):
            for plane in range(planes):
                for side in range(2):
                    pack_k[step, side, plane, pl.ds(i, 1), :] = field[step % 2, plane, i + 1, pl.ds((depth - 1) * side, 1), :]
            return 0

        lax.fori_loop(0, rows, row, 0)

    def send_sides(step):
        for side in range(2):
            @pl.when(has[1][side])
            def _():
                copy_i(step, side).start()

        for side in range(2):
            @pl.when(has[2][side])
            def _():
                copy_k(step, side).start()

    def wait_sides(step):
        for side in range(2):
            @pl.when(has[1][1 - side])
            def _():
                copy_i(step, side).wait_recv()

            @pl.when(has[2][1 - side])
            def _():
                copy_k(step, side).wait_recv()

    def wait_sides_sent(step):
        for side in range(2):
            @pl.when(has[1][side])
            def _():
                copy_i(step, side).wait_send()

            @pl.when(has[2][side])
            def _():
                copy_k(step, side).wait_send()

    def send_piece(step, piece):
        for side in range(2):
            @pl.when(has[0][side])
            def _():
                copy_j(step, piece, side).start()

    def wait_piece_sent(step, piece):
        for side in range(2):
            @pl.when(has[0][side])
            def _():
                copy_j(step, piece, side).wait_send()

    def wait_piece(step, piece):
        for side in range(2):
            @pl.when(has[0][1 - side])
            def _():
                copy_j(step, piece, side).wait_recv()

    def each(count, body):
        def one(index, _):
            body(index)
            return 0

        if count:
            lax.fori_loop(0, count, one, 0)

    for piece in range(len(pieces[0])):
        loads[2 * piece].wait()
        loads[2 * piece + 1].wait()
        send_piece(0, piece)

    for side in range(2):
        @pl.when(jnp.logical_not(has[1][side]))
        def _():
            for slot in range(2):
                field[slot, :, (rows + 1) * side] = jnp.zeros((planes, depth, 128), jnp.float32)

        @pl.when(jnp.logical_not(has[2][side]))
        def _():
            for step in range(STEPS):
                for plane in range(planes):
                    halo_k[step, side, plane] = jnp.zeros((rows, 128), jnp.float32)

        @pl.when(jnp.logical_not(has[0][side]))
        def _():
            def row(i, _):
                halo_j[0, side, i] = jnp.zeros((depth, 128), jnp.float32)
                return 0

            lax.fori_loop(0, rows, row, 0)

    loads[4].wait()
    pack(0)
    send_sides(0)
    loads[5].wait()
    for load in loads[6:]:
        load.wait()

    level = lax.broadcasted_iota(jnp.int32, (depth, 128), 0)
    first, last = level == 0, level == depth - 1

    def compute_row(step, i, to_face=False):
        old, new = step % 2, (step + 1) % 2
        slots = [jnp.where(has[0][side], step, 0) for side in range(2)]
        for plane in range(planes):
            here = field[old, plane, i + 1]
            terms = []
            if plane > 0:
                terms.append(field[old, plane - 1, i + 1])
            elif step < STEPS - 1:
                terms.append(halo_j[slots[0], 0, i])
            if plane < planes - 1:
                terms.append(field[old, plane + 1, i + 1])
            elif step < STEPS - 1:
                terms.append(halo_j[slots[1], 1, i])
            terms += [field[old, plane, i], field[old, plane, i + 2]]
            terms.append(jnp.where(first, halo_k[step, 0, plane, pl.ds(i, 1), :], pltpu.roll(here, 1, 0)))
            terms.append(jnp.where(last, halo_k[step, 1, plane, pl.ds(i, 1), :], pltpu.roll(here, depth - 1, 0)))
            spread = functools.reduce(jnp.add, terms) - 6.0 * here
            later = 2.0 * here - field[new, plane, i + 1] + speed[plane, i] * spread
            if step < STEPS - 1:
                field[new, plane, i + 1] = later
                if to_face and plane in (0, planes - 1):
                    face_ref[plane // (planes - 1), i - begin] = later
            elif plane in (0, planes - 1):
                outer_ref[plane // (planes - 1), i] = later
            else:
                inner_ref[plane - 1, i] = later

    def add_halo(step, i):
        for side in range(2):
            plane = (planes - 1) * side
            slot = jnp.where(has[0][side], step, 0)
            outer_ref[side, i] = outer_ref[side, i] + speed[plane, i] * halo_j[slot, side, i]

    for step in range(STEPS - 1):
        wait_sides(step)
        if step > 0:
            wait_sides_sent(step - 1)
        sent = 0
        for piece, (at, size) in enumerate(pieces[step]):
            if step > 0:
                wait_piece_sent(step - 1, piece)
            wait_piece(step, piece)
            kept = min(max(begin - at, 0), size) if step == STEPS - 2 else size
            each(kept, lambda i: compute_row(step, at + i))
            each(size - kept, lambda i: compute_row(step, at + kept + i, True))
            while sent < len(pieces[step + 1]) and sum(pieces[step + 1][sent]) <= at + size:
                if step + 1 < STEPS - 1:
                    send_piece(step + 1, sent)
                else:
                    @pl.when(is_early(place[1], sent))
                    def _():
                        send_piece(step + 1, sent)

                sent += 1
        pack(step + 1)
        send_sides(step + 1)

    step = STEPS - 1
    wait_sides(step)
    each(rows, lambda i: compute_row(step, i))
    for piece in range(len(pieces[step - 1])):
        wait_piece_sent(step - 1, piece)
    for before in (step - 1, step):
        wait_sides_sent(before)
    for piece, (at, size) in enumerate(pieces[step]):
        @pl.when(is_early(place[1], piece))
        def _():
            wait_piece(step, piece)
            each(size, lambda i: add_halo(step, at + i))
            wait_piece_sent(step, piece)


def is_early(lon, piece):
    return jnp.where(lon % 2 == 0, EARLY[0], EARLY[1]) > piece


def rest_kernel(rows, outer_ref, face_ref, face_speed_ref, token_ref, rest_ref, halo, send, recv):
    del token_ref
    depth = face_ref.shape[2]
    pieces = cuts(STEPS - 1, rows)
    begin = pieces[min(EARLY)][0]
    at_lat, at_lon = lax.axis_index("lat"), lax.axis_index("lon")
    has = (at_lat > 0, at_lat < lax.axis_size("lat") - 1)
    towards = ({"lat": at_lat - 1}, {"lat": at_lat + 1})

    barrier = pltpu.get_barrier_semaphore()
    for side in range(2):
        @pl.when(has[side])
        def _():
            pl.semaphore_signal(barrier, inc=1, device_id=towards[side], device_id_type=MESH)

    pl.semaphore_wait(barrier, has[0].astype(jnp.int32) + has[1].astype(jnp.int32))

    def copy(piece, side):
        at, size = pieces[piece]
        return pltpu.make_async_remote_copy(
            src_ref=face_ref.at[side, pl.ds(at - begin, size)],
            dst_ref=halo.at[1 - side, pl.ds(at - begin, size)],
            send_sem=send.at[side, piece],
            recv_sem=recv.at[1 - side, piece],
            device_id=towards[side],
            device_id_type=MESH,
        )

    late = range(min(EARLY), len(pieces))
    for piece in late:
        for side in range(2):
            @pl.when(has[side] & jnp.logical_not(is_early(at_lon, piece)))
            def _():
                copy(piece, side).start()

    for side in range(2):
        @pl.when(jnp.logical_not(has[side]))
        def _():
            def row(i, _):
                halo[side, i] = jnp.zeros((depth, 128), jnp.float32)
                return 0

            lax.fori_loop(0, rows - begin, row, 0)

    for piece in late:
        at, size = pieces[piece]

        @pl.when(jnp.logical_not(is_early(at_lon, piece)))
        def _():
            for side in range(2):
                @pl.when(has[1 - side])
                def _():
                    copy(piece, side).wait_recv()

            def row(i, _):
                for side in range(2):
                    on = at - begin + i
                    rest_ref[side, on] = outer_ref[side, at + i] + face_speed_ref[side, on] * halo[side, on]
                return 0

            lax.fori_loop(0, size, row, 0)

    for piece in late:
        for side in range(2):
            @pl.when(has[side] & jnp.logical_not(is_early(at_lon, piece)))
            def _():
                copy(piece, side).wait_send()


def run(copies):
    for condition, copy in copies:
        @pl.when(condition)
        def _():
            copy.start()

    for condition, copy in copies:
        @pl.when(condition)
        def _():
            copy.wait()


def write_early(inner_ref, outer_ref, out_ref, token_ref, sem):
    planes, rows = out_ref.shape[:2]
    lon = lax.axis_index("lon")
    copies = [
        (lon >= 0, pltpu.make_async_copy(inner_ref.at[plane], out_ref.at[plane + 1], sem.at[plane]))
        for plane in range(planes - 2)
    ]
    for piece, (at, size) in enumerate(cuts(STEPS - 1, rows)[:max(EARLY)]):
        for side in range(2):
            copies.append((is_early(lon, piece), pltpu.make_async_copy(
                outer_ref.at[side, pl.ds(at, size)],
                out_ref.at[(planes - 1) * side, pl.ds(at, size)],
                sem.at[len(copies)],
            )))
    run(copies)
    token_ref[...] = jnp.zeros_like(token_ref)


def write_rest(rest_ref, begun_ref, out_ref, sem):
    del begun_ref
    planes, rows = out_ref.shape[:2]
    lon = lax.axis_index("lon")
    pieces = cuts(STEPS - 1, rows)
    begin = pieces[min(EARLY)][0]
    spans = [
        (side, at, size, jnp.logical_not(is_early(lon, piece)))
        for piece, (at, size) in enumerate(pieces) if piece >= min(EARLY) for side in range(2)
    ]
    run([
        (condition, pltpu.make_async_copy(
            rest_ref.at[side, pl.ds(at - begin, size)],
            out_ref.at[(planes - 1) * side, pl.ds(at, size)],
            sem.at[index]))
        for index, (side, at, size, condition) in enumerate(spans)
    ])


def local(field_now, earlier, speed_square):
    planes, rows, depth, members = field_now.shape
    shape, f32 = field_now.shape, jnp.float32
    begin = cuts(STEPS - 1, rows)[min(EARLY)][0]
    most = max(map(len, PIECES))
    in_hbm, in_vmem = pl.BlockSpec(memory_space=pl.ANY), pl.BlockSpec(memory_space=pltpu.VMEM)
    dma = pltpu.SemaphoreType.DMA
    inner, outer, face, face_speed = pl.pallas_call(
        kernel,
        out_shape=(
            pltpu.VMEM((planes - 2, rows, depth, members), f32),
            pltpu.VMEM((2, rows, depth, members), f32),
            pltpu.VMEM((2, rows - begin, depth, members), f32),
            pltpu.VMEM((2, rows - begin, depth, members), f32),
        ),
        in_specs=[in_hbm] * 3,
        out_specs=(in_vmem,) * 4,
        scratch_shapes=[
            pltpu.VMEM((2, planes, rows + 2, depth, members), f32),
            pltpu.VMEM(shape, f32),
            pltpu.VMEM((STEPS, 2, rows, depth, members), f32),
            pltpu.VMEM((STEPS, 2, planes, rows, members), f32),
            pltpu.VMEM((STEPS, 2, planes, rows, members), f32),
            dma((9,)),
            dma((STEPS, 2, most)),
            dma((STEPS, 2, most)),
            dma((STEPS, 2)),
            dma((STEPS, 2)),
            dma((STEPS, 2)),
            dma((STEPS, 2)),
        ],
        compiler_params=pltpu.CompilerParams(
            collective_id=0, has_side_effects=True, vmem_limit_bytes=46 * 2**20
        ),
    )(field_now, earlier, speed_square)
    begun, token = pl.pallas_call(
        write_early,
        out_shape=(jax.ShapeDtypeStruct(shape, f32), pltpu.VMEM((8, 128), f32)),
        in_specs=[in_vmem] * 2,
        out_specs=(in_hbm, in_vmem),
        scratch_shapes=[dma((planes - 2 + 2 * max(EARLY),))],
        compiler_params=pltpu.CompilerParams(vmem_limit_bytes=2**20),
    )(inner, outer)
    rest = pl.pallas_call(
        functools.partial(rest_kernel, rows),
        out_shape=pltpu.VMEM((2, rows - begin, depth, members), f32),
        in_specs=[in_vmem] * 4,
        out_specs=in_vmem,
        scratch_shapes=[
            pltpu.VMEM((2, rows - begin, depth, members), f32),
            dma((2, most)),
            dma((2, most)),
        ],
        compiler_params=pltpu.CompilerParams(
            collective_id=1, has_side_effects=True, vmem_limit_bytes=8 * 2**20
        ),
    )(outer, face, face_speed, token)
    return pl.pallas_call(
        write_rest,
        out_shape=jax.ShapeDtypeStruct(shape, f32),
        in_specs=[in_vmem, in_hbm],
        out_specs=in_hbm,
        input_output_aliases={1: 0},
        scratch_shapes=[dma((2 * most,))],
        compiler_params=pltpu.CompilerParams(vmem_limit_bytes=2**20),
    )(rest, begun)


def solution(mesh):
    spec = P("lat", "lon", "lev", None)
    return jax.shard_map(local, mesh=mesh, in_specs=(spec,) * 3, out_specs=spec, check_vma=False)
```

```python
import functools

import jax
import jax.numpy as jnp
from jax import lax
from jax.experimental import pallas as pl
from jax.experimental.pallas import tpu as pltpu
from jax.sharding import PartitionSpec as P

STEPS = 4
PIECES = ((32, 32), (32, 32), (32, 32), (28, 30, 6))
EARLY = (1, 2)
MESH = pl.DeviceIdType.MESH


def cuts(step, rows):
    sizes = [size * rows // sum(PIECES[step]) for size in PIECES[step]]
    return [(sum(sizes[:index]), size) for index, size in enumerate(sizes)]


def kernel(
    now_ref, earlier_ref, speed_ref, inner_ref, outer_ref, face_ref, face_speed_ref, field, speed, halo_j, halo_k, pack_k,
    met_sem, load_sem, send_j, recv_j, send_i, recv_i, send_k, recv_k,
):
    planes, rows, depth, _ = now_ref.shape
    pieces = [cuts(step, rows) for step in range(STEPS)]
    begin = pieces[-1][min(EARLY)][0]
    place = [lax.axis_index(axis) for axis in ("lat", "lon", "lev")]
    sizes = [lax.axis_size(axis) for axis in ("lat", "lon", "lev")]
    has = [(at > 0, at < size - 1) for at, size in zip(place, sizes)]
    towards = [
        tuple({axis: at + shift} for shift in (-1, 1))
        for axis, at in zip(("lat", "lon", "lev"), place)
    ]

    lat, lon, lev = place
    x_lo, x_hi = lon // 2, lev % 2
    beside = [
        (x_lo + x_hi > 0, {"lon": lon + 2 - 4 * x_lo, "lev": lev - 1 + x_lo}),
        (x_lo + x_hi < 2, {"lon": lon + 2 - 4 * x_lo, "lev": lev + x_lo}),
        (lev >= 2, {"lev": lev - 2}),
        (lev < sizes[2] - 2, {"lev": lev + 2}),
        (lon >= 0, {"lon": lon + 1 - 2 * (lon % 2)}),
    ]

    def greet(semaphore, devices):
        count = 0
        for there, device in devices:
            count = count + there.astype(jnp.int32)

            @pl.when(there)
            def _():
                pl.semaphore_signal(semaphore, inc=1, device_id=device, device_id_type=MESH)

        return count

    barrier = pltpu.get_barrier_semaphore()
    count = greet(barrier, beside + [(has[0][side], towards[0][side]) for side in range(2)])

    spans = [(plane, 1, at, size) for at, size in pieces[0] for plane in (0, planes - 1)]
    spans.append((1, planes - 2, 0, rows))
    loads = [
        pltpu.make_async_copy(
            now_ref.at[pl.ds(plane, count), pl.ds(at, size)],
            field.at[0, pl.ds(plane, count), pl.ds(at + 1, size)],
            load_sem.at[index],
        )
        for index, (plane, count, at, size) in enumerate(spans)
    ]
    loads.append(pltpu.make_async_copy(earlier_ref, field.at[1, :, pl.ds(1, rows)], load_sem.at[5]))
    loads.append(pltpu.make_async_copy(speed_ref, speed, load_sem.at[6]))
    loads += [
        pltpu.make_async_copy(
            speed_ref.at[(planes - 1) * side, pl.ds(begin, rows - begin)], face_speed_ref.at[side], load_sem.at[7 + side]
        )
        for side in range(2)
    ]
    for load in loads:
        load.start()

    pl.semaphore_wait(barrier, count)

    def copy_j(step, piece, side):
        at, size = pieces[step][piece]
        if step == STEPS - 1 and at >= begin:
            source = face_ref.at[side, pl.ds(at - begin, size)]
        else:
            source = field.at[step % 2, (planes - 1) * side, pl.ds(at + 1, size)]
        return pltpu.make_async_remote_copy(
            src_ref=source,
            dst_ref=halo_j.at[step, 1 - side, pl.ds(at, size)],
            send_sem=send_j.at[step, side, piece],
            recv_sem=recv_j.at[step, 1 - side, piece],
            device_id=towards[0][side],
            device_id_type=MESH,
        )

    def copy_i(step, side):
        return pltpu.make_async_remote_copy(
            src_ref=field.at[step % 2, :, 1 + (rows - 1) * side],
            dst_ref=field.at[step % 2, :, (rows + 1) * (1 - side)],
            send_sem=send_i.at[step, side],
            recv_sem=recv_i.at[step, 1 - side],
            device_id=towards[1][side],
            device_id_type=MESH,
        )

    def copy_k(step, side):
        return pltpu.make_async_remote_copy(
            src_ref=pack_k.at[step, side],
            dst_ref=halo_k.at[step, 1 - side],
            send_sem=send_k.at[step, side],
            recv_sem=recv_k.at[step, 1 - side],
            device_id=towards[2][side],
            device_id_type=MESH,
        )

    def pack(step):
        def row(i, _):
            for plane in range(planes):
                for side in range(2):
                    pack_k[step, side, plane, pl.ds(i, 1), :] = field[step % 2, plane, i + 1, pl.ds((depth - 1) * side, 1), :]
            return 0

        lax.fori_loop(0, rows, row, 0)

    def send_sides(step):
        for side in range(2):
            @pl.when(has[1][side])
            def _():
                copy_i(step, side).start()

        for side in range(2):
            @pl.when(has[2][side])
            def _():
                copy_k(step, side).start()

    def wait_sides(step):
        for side in range(2):
            @pl.when(has[1][1 - side])
            def _():
                copy_i(step, side).wait_recv()

            @pl.when(has[2][1 - side])
            def _():
                copy_k(step, side).wait_recv()

    def wait_sides_sent(step):
        for side in range(2):
            @pl.when(has[1][side])
            def _():
                copy_i(step, side).wait_send()

            @pl.when(has[2][side])
            def _():
                copy_k(step, side).wait_send()

    def send_piece(step, piece):
        for side in range(2):
            @pl.when(has[0][side])
            def _():
                copy_j(step, piece, side).start()

    def wait_piece_sent(step, piece):
        for side in range(2):
            @pl.when(has[0][side])
            def _():
                copy_j(step, piece, side).wait_send()

    def wait_piece(step, piece):
        for side in range(2):
            @pl.when(has[0][1 - side])
            def _():
                copy_j(step, piece, side).wait_recv()

    def each(count, body):
        def one(index, _):
            body(index)
            return 0

        if count:
            lax.fori_loop(0, count, one, 0)

    for piece in range(len(pieces[0])):
        loads[2 * piece].wait()
        loads[2 * piece + 1].wait()
        send_piece(0, piece)

    for index in range(2):
        pl.semaphore_wait(met_sem.at[index], greet(met_sem.at[index], beside))

    for side in range(2):
        @pl.when(jnp.logical_not(has[1][side]))
        def _():
            for slot in range(2):
                field[slot, :, (rows + 1) * side] = jnp.zeros((planes, depth, 128), jnp.float32)

        @pl.when(jnp.logical_not(has[2][side]))
        def _():
            for step in range(STEPS):
                for plane in range(planes):
                    halo_k[step, side, plane] = jnp.zeros((rows, 128), jnp.float32)

        @pl.when(jnp.logical_not(has[0][side]))
        def _():
            def row(i, _):
                halo_j[0, side, i] = jnp.zeros((depth, 128), jnp.float32)
                return 0

            lax.fori_loop(0, rows, row, 0)

    loads[4].wait()
    pack(0)
    send_sides(0)
    loads[5].wait()
    for load in loads[6:]:
        load.wait()

    level = lax.broadcasted_iota(jnp.int32, (depth, 128), 0)
    first, last = level == 0, level == depth - 1

    def compute_row(step, i, to_face=False):
        old, new = step % 2, (step + 1) % 2
        slots = [jnp.where(has[0][side], step, 0) for side in range(2)]
        for plane in range(planes):
            here = field[old, plane, i + 1]
            terms = []
            if plane > 0:
                terms.append(field[old, plane - 1, i + 1])
            elif step < STEPS - 1:
                terms.append(halo_j[slots[0], 0, i])
            if plane < planes - 1:
                terms.append(field[old, plane + 1, i + 1])
            elif step < STEPS - 1:
                terms.append(halo_j[slots[1], 1, i])
            terms += [field[old, plane, i], field[old, plane, i + 2]]
            terms.append(jnp.where(first, halo_k[step, 0, plane, pl.ds(i, 1), :], pltpu.roll(here, 1, 0)))
            terms.append(jnp.where(last, halo_k[step, 1, plane, pl.ds(i, 1), :], pltpu.roll(here, depth - 1, 0)))
            spread = functools.reduce(jnp.add, terms) - 6.0 * here
            later = 2.0 * here - field[new, plane, i + 1] + speed[plane, i] * spread
            if step < STEPS - 1:
                field[new, plane, i + 1] = later
                if to_face and plane in (0, planes - 1):
                    face_ref[plane // (planes - 1), i - begin] = later
            elif plane in (0, planes - 1):
                outer_ref[plane // (planes - 1), i] = later
            else:
                inner_ref[plane - 1, i] = later

    def add_halo(step, i):
        for side in range(2):
            plane = (planes - 1) * side
            slot = jnp.where(has[0][side], step, 0)
            outer_ref[side, i] = outer_ref[side, i] + speed[plane, i] * halo_j[slot, side, i]

    for step in range(STEPS - 1):
        wait_sides(step)
        if step > 0:
            wait_sides_sent(step - 1)
        sent = 0
        for piece, (at, size) in enumerate(pieces[step]):
            if step > 0:
                wait_piece_sent(step - 1, piece)
            wait_piece(step, piece)
            kept = min(max(begin - at, 0), size) if step == STEPS - 2 else size
            each(kept, lambda i: compute_row(step, at + i))
            each(size - kept, lambda i: compute_row(step, at + kept + i, True))
            while sent < len(pieces[step + 1]) and sum(pieces[step + 1][sent]) <= at + size:
                if step + 1 < STEPS - 1:
                    send_piece(step + 1, sent)
                else:
                    @pl.when(is_early(place[1], sent))
                    def _():
                        send_piece(step + 1, sent)

                sent += 1
        pack(step + 1)
        send_sides(step + 1)

    step = STEPS - 1
    wait_sides(step)
    each(rows, lambda i: compute_row(step, i))
    for piece in range(len(pieces[step - 1])):
        wait_piece_sent(step - 1, piece)
    for before in (step - 1, step):
        wait_sides_sent(before)
    for piece, (at, size) in enumerate(pieces[step]):
        @pl.when(is_early(place[1], piece))
        def _():
            wait_piece(step, piece)
            each(size, lambda i: add_halo(step, at + i))
            wait_piece_sent(step, piece)


def is_early(lon, piece):
    return jnp.where(lon % 2 == 0, EARLY[0], EARLY[1]) > piece


def rest_kernel(rows, outer_ref, face_ref, face_speed_ref, token_ref, rest_ref, halo, send, recv):
    del token_ref
    depth = face_ref.shape[2]
    pieces = cuts(STEPS - 1, rows)
    begin = pieces[min(EARLY)][0]
    at_lat, at_lon = lax.axis_index("lat"), lax.axis_index("lon")
    has = (at_lat > 0, at_lat < lax.axis_size("lat") - 1)
    towards = ({"lat": at_lat - 1}, {"lat": at_lat + 1})

    barrier = pltpu.get_barrier_semaphore()
    for side in range(2):
        @pl.when(has[side])
        def _():
            pl.semaphore_signal(barrier, inc=1, device_id=towards[side], device_id_type=MESH)

    pl.semaphore_wait(barrier, has[0].astype(jnp.int32) + has[1].astype(jnp.int32))

    def copy(piece, side):
        at, size = pieces[piece]
        return pltpu.make_async_remote_copy(
            src_ref=face_ref.at[side, pl.ds(at - begin, size)],
            dst_ref=halo.at[1 - side, pl.ds(at - begin, size)],
            send_sem=send.at[side, piece],
            recv_sem=recv.at[1 - side, piece],
            device_id=towards[side],
            device_id_type=MESH,
        )

    late = range(min(EARLY), len(pieces))
    for piece in late:
        for side in range(2):
            @pl.when(has[side] & jnp.logical_not(is_early(at_lon, piece)))
            def _():
                copy(piece, side).start()

    for side in range(2):
        @pl.when(jnp.logical_not(has[side]))
        def _():
            def row(i, _):
                halo[side, i] = jnp.zeros((depth, 128), jnp.float32)
                return 0

            lax.fori_loop(0, rows - begin, row, 0)

    for piece in late:
        at, size = pieces[piece]

        @pl.when(jnp.logical_not(is_early(at_lon, piece)))
        def _():
            for side in range(2):
                @pl.when(has[1 - side])
                def _():
                    copy(piece, side).wait_recv()

            def row(i, _):
                for side in range(2):
                    on = at - begin + i
                    rest_ref[side, on] = outer_ref[side, at + i] + face_speed_ref[side, on] * halo[side, on]
                return 0

            lax.fori_loop(0, size, row, 0)

    for piece in late:
        for side in range(2):
            @pl.when(has[side] & jnp.logical_not(is_early(at_lon, piece)))
            def _():
                copy(piece, side).wait_send()


def run(copies):
    for condition, copy in copies:
        @pl.when(condition)
        def _():
            copy.start()

    for condition, copy in copies:
        @pl.when(condition)
        def _():
            copy.wait()


def write_early(inner_ref, outer_ref, out_ref, token_ref, sem):
    planes, rows = out_ref.shape[:2]
    lon = lax.axis_index("lon")
    copies = [
        (lon >= 0, pltpu.make_async_copy(inner_ref.at[plane], out_ref.at[plane + 1], sem.at[plane]))
        for plane in range(planes - 2)
    ]
    for piece, (at, size) in enumerate(cuts(STEPS - 1, rows)[:max(EARLY)]):
        for side in range(2):
            copies.append((is_early(lon, piece), pltpu.make_async_copy(
                outer_ref.at[side, pl.ds(at, size)],
                out_ref.at[(planes - 1) * side, pl.ds(at, size)],
                sem.at[len(copies)],
            )))
    run(copies)
    token_ref[...] = jnp.zeros_like(token_ref)


def write_rest(rest_ref, begun_ref, out_ref, sem):
    del begun_ref
    planes, rows = out_ref.shape[:2]
    lon = lax.axis_index("lon")
    pieces = cuts(STEPS - 1, rows)
    begin = pieces[min(EARLY)][0]
    spans = [
        (side, at, size, jnp.logical_not(is_early(lon, piece)))
        for piece, (at, size) in enumerate(pieces) if piece >= min(EARLY) for side in range(2)
    ]
    run([
        (condition, pltpu.make_async_copy(
            rest_ref.at[side, pl.ds(at - begin, size)],
            out_ref.at[(planes - 1) * side, pl.ds(at, size)],
            sem.at[index]))
        for index, (side, at, size, condition) in enumerate(spans)
    ])


def local(field_now, earlier, speed_square):
    planes, rows, depth, members = field_now.shape
    shape, f32 = field_now.shape, jnp.float32
    begin = cuts(STEPS - 1, rows)[min(EARLY)][0]
    most = max(map(len, PIECES))
    in_hbm, in_vmem = pl.BlockSpec(memory_space=pl.ANY), pl.BlockSpec(memory_space=pltpu.VMEM)
    dma = pltpu.SemaphoreType.DMA
    inner, outer, face, face_speed = pl.pallas_call(
        kernel,
        out_shape=(
            pltpu.VMEM((planes - 2, rows, depth, members), f32),
            pltpu.VMEM((2, rows, depth, members), f32),
            pltpu.VMEM((2, rows - begin, depth, members), f32),
            pltpu.VMEM((2, rows - begin, depth, members), f32),
        ),
        in_specs=[in_hbm] * 3,
        out_specs=(in_vmem,) * 4,
        scratch_shapes=[
            pltpu.VMEM((2, planes, rows + 2, depth, members), f32),
            pltpu.VMEM(shape, f32),
            pltpu.VMEM((STEPS, 2, rows, depth, members), f32),
            pltpu.VMEM((STEPS, 2, planes, rows, members), f32),
            pltpu.VMEM((STEPS, 2, planes, rows, members), f32),
            pltpu.SemaphoreType.REGULAR((2,)),
            dma((9,)),
            dma((STEPS, 2, most)),
            dma((STEPS, 2, most)),
            dma((STEPS, 2)),
            dma((STEPS, 2)),
            dma((STEPS, 2)),
            dma((STEPS, 2)),
        ],
        compiler_params=pltpu.CompilerParams(
            collective_id=0, has_side_effects=True, vmem_limit_bytes=46 * 2**20
        ),
    )(field_now, earlier, speed_square)
    begun, token = pl.pallas_call(
        write_early,
        out_shape=(jax.ShapeDtypeStruct(shape, f32), pltpu.VMEM((8, 128), f32)),
        in_specs=[in_vmem] * 2,
        out_specs=(in_hbm, in_vmem),
        scratch_shapes=[dma((planes - 2 + 2 * max(EARLY),))],
        compiler_params=pltpu.CompilerParams(vmem_limit_bytes=2**20),
    )(inner, outer)
    rest = pl.pallas_call(
        functools.partial(rest_kernel, rows),
        out_shape=pltpu.VMEM((2, rows - begin, depth, members), f32),
        in_specs=[in_vmem] * 4,
        out_specs=in_vmem,
        scratch_shapes=[
            pltpu.VMEM((2, rows - begin, depth, members), f32),
            dma((2, most)),
            dma((2, most)),
        ],
        compiler_params=pltpu.CompilerParams(
            collective_id=1, has_side_effects=True, vmem_limit_bytes=8 * 2**20
        ),
    )(outer, face, face_speed, token)
    return pl.pallas_call(
        write_rest,
        out_shape=jax.ShapeDtypeStruct(shape, f32),
        in_specs=[in_vmem, in_hbm],
        out_specs=in_hbm,
        input_output_aliases={1: 0},
        scratch_shapes=[dma((2 * most,))],
        compiler_params=pltpu.CompilerParams(vmem_limit_bytes=2**20),
    )(rest, begun)


def solution(mesh):
    spec = P("lat", "lon", "lev", None)
    return jax.shard_map(local, mesh=mesh, in_specs=(spec,) * 3, out_specs=spec, check_vma=False)
```

```python
import functools

import jax
import jax.numpy as jnp
from jax import lax
from jax.experimental import pallas as pl
from jax.experimental.pallas import tpu as pltpu
from jax.sharding import PartitionSpec as P

STEPS = 4
PIECES = ((32, 32), (32, 32), (32, 32), (28, 30, 6))
EARLY = (1, 2)
MESH = pl.DeviceIdType.MESH


def cuts(step, rows):
    sizes = [size * rows // sum(PIECES[step]) for size in PIECES[step]]
    return [(sum(sizes[:index]), size) for index, size in enumerate(sizes)]


def kernel(
    now_ref, earlier_ref, speed_ref, inner_ref, outer_ref, face_ref, face_speed_ref, field, speed, halo_j, halo_k, pack_k,
    met_sem, load_sem, send_j, recv_j, send_i, recv_i, send_k, recv_k,
):
    planes, rows, depth, _ = now_ref.shape
    pieces = [cuts(step, rows) for step in range(STEPS)]
    begin = pieces[-1][min(EARLY)][0]
    place = [lax.axis_index(axis) for axis in ("lat", "lon", "lev")]
    sizes = [lax.axis_size(axis) for axis in ("lat", "lon", "lev")]
    has = [(at > 0, at < size - 1) for at, size in zip(place, sizes)]
    towards = [
        tuple({axis: at + shift} for shift in (-1, 1))
        for axis, at in zip(("lat", "lon", "lev"), place)
    ]

    lat, lon, lev = place
    x_lo, x_hi = lon // 2, lev % 2
    beside = [
        (x_lo + x_hi > 0, {"lon": lon + 2 - 4 * x_lo, "lev": lev - 1 + x_lo}),
        (x_lo + x_hi < 2, {"lon": lon + 2 - 4 * x_lo, "lev": lev + x_lo}),
        (lev >= 2, {"lev": lev - 2}),
        (lev < sizes[2] - 2, {"lev": lev + 2}),
        (lon >= 0, {"lon": lon + 1 - 2 * (lon % 2)}),
    ]

    def greet(semaphore, devices):
        count = 0
        for there, device in devices:
            count = count + there.astype(jnp.int32)

            @pl.when(there)
            def _():
                pl.semaphore_signal(semaphore, inc=1, device_id=device, device_id_type=MESH)

        return count

    barrier = pltpu.get_barrier_semaphore()
    count = greet(barrier, beside + [(has[0][side], towards[0][side]) for side in range(2)])

    faces = 2 * len(pieces[0])
    spans = [(plane, 1, at, size) for at, size in pieces[0] for plane in (0, planes - 1)]
    spans.append((1, planes - 2, 0, rows))
    loads = [
        pltpu.make_async_copy(
            now_ref.at[pl.ds(plane, count), pl.ds(at, size)],
            field.at[0, pl.ds(plane, count), pl.ds(at + 1, size)],
            load_sem.at[index],
        )
        for index, (plane, count, at, size) in enumerate(spans)
    ]
    loads.append(pltpu.make_async_copy(earlier_ref, field.at[1, :, pl.ds(1, rows)], load_sem.at[faces + 1]))
    loads.append(pltpu.make_async_copy(speed_ref, speed, load_sem.at[faces + 2]))
    loads += [
        pltpu.make_async_copy(
            speed_ref.at[(planes - 1) * side, pl.ds(begin, rows - begin)], face_speed_ref.at[side], load_sem.at[faces + 3 + side]
        )
        for side in range(2)
    ]
    for load in loads[:faces]:
        load.start()

    pl.semaphore_wait(barrier, count)

    def copy_j(step, piece, side):
        at, size = pieces[step][piece]
        if step == STEPS - 1 and at >= begin:
            source = face_ref.at[side, pl.ds(at - begin, size)]
        else:
            source = field.at[step % 2, (planes - 1) * side, pl.ds(at + 1, size)]
        return pltpu.make_async_remote_copy(
            src_ref=source,
            dst_ref=halo_j.at[step, 1 - side, pl.ds(at, size)],
            send_sem=send_j.at[step, side, piece],
            recv_sem=recv_j.at[step, 1 - side, piece],
            device_id=towards[0][side],
            device_id_type=MESH,
        )

    def copy_i(step, side):
        return pltpu.make_async_remote_copy(
            src_ref=field.at[step % 2, :, 1 + (rows - 1) * side],
            dst_ref=field.at[step % 2, :, (rows + 1) * (1 - side)],
            send_sem=send_i.at[step, side],
            recv_sem=recv_i.at[step, 1 - side],
            device_id=towards[1][side],
            device_id_type=MESH,
        )

    def copy_k(step, side):
        return pltpu.make_async_remote_copy(
            src_ref=pack_k.at[step, side],
            dst_ref=halo_k.at[step, 1 - side],
            send_sem=send_k.at[step, side],
            recv_sem=recv_k.at[step, 1 - side],
            device_id=towards[2][side],
            device_id_type=MESH,
        )

    def pack(step):
        def row(i, _):
            for plane in range(planes):
                for side in range(2):
                    pack_k[step, side, plane, pl.ds(i, 1), :] = field[step % 2, plane, i + 1, pl.ds((depth - 1) * side, 1), :]
            return 0

        lax.fori_loop(0, rows, row, 0)

    def send_sides(step):
        for side in range(2):
            @pl.when(has[1][side])
            def _():
                copy_i(step, side).start()

        for side in range(2):
            @pl.when(has[2][side])
            def _():
                copy_k(step, side).start()

    def wait_sides(step):
        for side in range(2):
            @pl.when(has[1][1 - side])
            def _():
                copy_i(step, side).wait_recv()

            @pl.when(has[2][1 - side])
            def _():
                copy_k(step, side).wait_recv()

    def wait_sides_sent(step):
        for side in range(2):
            @pl.when(has[1][side])
            def _():
                copy_i(step, side).wait_send()

            @pl.when(has[2][side])
            def _():
                copy_k(step, side).wait_send()

    def send_piece(step, piece):
        for side in range(2):
            @pl.when(has[0][side])
            def _():
                copy_j(step, piece, side).start()

    def wait_piece_sent(step, piece):
        for side in range(2):
            @pl.when(has[0][side])
            def _():
                copy_j(step, piece, side).wait_send()

    def wait_piece(step, piece):
        for side in range(2):
            @pl.when(has[0][1 - side])
            def _():
                copy_j(step, piece, side).wait_recv()

    def each(count, body):
        def one(index, _):
            body(index)
            return 0

        if count:
            lax.fori_loop(0, count, one, 0)

    for piece in range(len(pieces[0])):
        loads[2 * piece].wait()
        loads[2 * piece + 1].wait()
        send_piece(0, piece)

    for load in loads[faces:]:
        load.start()

    for index in range(2):
        pl.semaphore_wait(met_sem.at[index], greet(met_sem.at[index], beside))

    for side in range(2):
        @pl.when(jnp.logical_not(has[1][side]))
        def _():
            for slot in range(2):
                field[slot, :, (rows + 1) * side] = jnp.zeros((planes, depth, 128), jnp.float32)

        @pl.when(jnp.logical_not(has[2][side]))
        def _():
            for step in range(STEPS):
                for plane in range(planes):
                    halo_k[step, side, plane] = jnp.zeros((rows, 128), jnp.float32)

        @pl.when(jnp.logical_not(has[0][side]))
        def _():
            def row(i, _):
                halo_j[0, side, i] = jnp.zeros((depth, 128), jnp.float32)
                return 0

            lax.fori_loop(0, rows, row, 0)

    loads[faces].wait()
    pack(0)
    send_sides(0)
    for load in loads[faces + 1:]:
        load.wait()

    level = lax.broadcasted_iota(jnp.int32, (depth, 128), 0)
    first, last = level == 0, level == depth - 1

    def compute_row(step, i, to_face=False):
        old, new = step % 2, (step + 1) % 2
        slots = [jnp.where(has[0][side], step, 0) for side in range(2)]
        for plane in range(planes):
            here = field[old, plane, i + 1]
            terms = []
            if plane > 0:
                terms.append(field[old, plane - 1, i + 1])
            elif step < STEPS - 1:
                terms.append(halo_j[slots[0], 0, i])
            if plane < planes - 1:
                terms.append(field[old, plane + 1, i + 1])
            elif step < STEPS - 1:
                terms.append(halo_j[slots[1], 1, i])
            terms += [field[old, plane, i], field[old, plane, i + 2]]
            terms.append(jnp.where(first, halo_k[step, 0, plane, pl.ds(i, 1), :], pltpu.roll(here, 1, 0)))
            terms.append(jnp.where(last, halo_k[step, 1, plane, pl.ds(i, 1), :], pltpu.roll(here, depth - 1, 0)))
            spread = functools.reduce(jnp.add, terms) - 6.0 * here
            later = 2.0 * here - field[new, plane, i + 1] + speed[plane, i] * spread
            if step < STEPS - 1:
                field[new, plane, i + 1] = later
                if to_face and plane in (0, planes - 1):
                    face_ref[plane // (planes - 1), i - begin] = later
            elif plane in (0, planes - 1):
                outer_ref[plane // (planes - 1), i] = later
            else:
                inner_ref[plane - 1, i] = later

    def add_halo(step, i):
        for side in range(2):
            plane = (planes - 1) * side
            slot = jnp.where(has[0][side], step, 0)
            outer_ref[side, i] = outer_ref[side, i] + speed[plane, i] * halo_j[slot, side, i]

    for step in range(STEPS - 1):
        wait_sides(step)
        if step > 0:
            wait_sides_sent(step - 1)
        sent = free = 0
        for piece, (at, size) in enumerate(pieces[step]):
            while step > 0 and free < len(pieces[step - 1]) and pieces[step - 1][free][0] < at + size:
                wait_piece_sent(step - 1, free)
                free += 1
            wait_piece(step, piece)
            kept = min(max(begin - at, 0), size) if step == STEPS - 2 else size
            each(kept, lambda i: compute_row(step, at + i))
            each(size - kept, lambda i: compute_row(step, at + kept + i, True))
            while sent < len(pieces[step + 1]) and sum(pieces[step + 1][sent]) <= at + size:
                if step + 1 < STEPS - 1:
                    send_piece(step + 1, sent)
                else:
                    @pl.when(is_early(place[1], sent))
                    def _():
                        send_piece(step + 1, sent)

                sent += 1
        pack(step + 1)
        send_sides(step + 1)

    step = STEPS - 1
    wait_sides(step)
    each(rows, lambda i: compute_row(step, i))
    for piece in range(len(pieces[step - 1])):
        wait_piece_sent(step - 1, piece)
    for before in (step - 1, step):
        wait_sides_sent(before)
    for piece, (at, size) in enumerate(pieces[step]):
        @pl.when(is_early(place[1], piece))
        def _():
            wait_piece(step, piece)
            each(size, lambda i: add_halo(step, at + i))
            wait_piece_sent(step, piece)


def is_early(lon, piece):
    return jnp.where(lon % 2 == 0, EARLY[0], EARLY[1]) > piece


def rest_kernel(rows, outer_ref, face_ref, face_speed_ref, token_ref, rest_ref, halo, send, recv):
    del token_ref
    depth = face_ref.shape[2]
    pieces = cuts(STEPS - 1, rows)
    begin = pieces[min(EARLY)][0]
    at_lat, at_lon = lax.axis_index("lat"), lax.axis_index("lon")
    has = (at_lat > 0, at_lat < lax.axis_size("lat") - 1)
    towards = ({"lat": at_lat - 1}, {"lat": at_lat + 1})

    barrier = pltpu.get_barrier_semaphore()
    for side in range(2):
        @pl.when(has[side])
        def _():
            pl.semaphore_signal(barrier, inc=1, device_id=towards[side], device_id_type=MESH)

    pl.semaphore_wait(barrier, has[0].astype(jnp.int32) + has[1].astype(jnp.int32))

    def copy(piece, side):
        at, size = pieces[piece]
        return pltpu.make_async_remote_copy(
            src_ref=face_ref.at[side, pl.ds(at - begin, size)],
            dst_ref=halo.at[1 - side, pl.ds(at - begin, size)],
            send_sem=send.at[side, piece],
            recv_sem=recv.at[1 - side, piece],
            device_id=towards[side],
            device_id_type=MESH,
        )

    late = range(min(EARLY), len(pieces))
    for piece in late:
        for side in range(2):
            @pl.when(has[side] & jnp.logical_not(is_early(at_lon, piece)))
            def _():
                copy(piece, side).start()

    for side in range(2):
        @pl.when(jnp.logical_not(has[side]))
        def _():
            def row(i, _):
                halo[side, i] = jnp.zeros((depth, 128), jnp.float32)
                return 0

            lax.fori_loop(0, rows - begin, row, 0)

    for piece in late:
        at, size = pieces[piece]

        @pl.when(jnp.logical_not(is_early(at_lon, piece)))
        def _():
            for side in range(2):
                @pl.when(has[1 - side])
                def _():
                    copy(piece, side).wait_recv()

            def row(i, _):
                for side in range(2):
                    on = at - begin + i
                    rest_ref[side, on] = outer_ref[side, at + i] + face_speed_ref[side, on] * halo[side, on]
                return 0

            lax.fori_loop(0, size, row, 0)

    for piece in late:
        for side in range(2):
            @pl.when(has[side] & jnp.logical_not(is_early(at_lon, piece)))
            def _():
                copy(piece, side).wait_send()


def run(copies):
    for condition, copy in copies:
        @pl.when(condition)
        def _():
            copy.start()

    for condition, copy in copies:
        @pl.when(condition)
        def _():
            copy.wait()


def write_early(inner_ref, outer_ref, out_ref, token_ref, sem):
    planes, rows = out_ref.shape[:2]
    lon = lax.axis_index("lon")
    copies = [
        (lon >= 0, pltpu.make_async_copy(inner_ref.at[plane], out_ref.at[plane + 1], sem.at[plane]))
        for plane in range(planes - 2)
    ]
    for piece, (at, size) in enumerate(cuts(STEPS - 1, rows)[:max(EARLY)]):
        for side in range(2):
            copies.append((is_early(lon, piece), pltpu.make_async_copy(
                outer_ref.at[side, pl.ds(at, size)],
                out_ref.at[(planes - 1) * side, pl.ds(at, size)],
                sem.at[len(copies)],
            )))
    run(copies)
    token_ref[...] = jnp.zeros_like(token_ref)


def write_rest(rest_ref, begun_ref, out_ref, sem):
    del begun_ref
    planes, rows = out_ref.shape[:2]
    lon = lax.axis_index("lon")
    pieces = cuts(STEPS - 1, rows)
    begin = pieces[min(EARLY)][0]
    spans = [
        (side, at, size, jnp.logical_not(is_early(lon, piece)))
        for piece, (at, size) in enumerate(pieces) if piece >= min(EARLY) for side in range(2)
    ]
    run([
        (condition, pltpu.make_async_copy(
            rest_ref.at[side, pl.ds(at - begin, size)],
            out_ref.at[(planes - 1) * side, pl.ds(at, size)],
            sem.at[index]))
        for index, (side, at, size, condition) in enumerate(spans)
    ])


def local(field_now, earlier, speed_square):
    planes, rows, depth, members = field_now.shape
    shape, f32 = field_now.shape, jnp.float32
    begin = cuts(STEPS - 1, rows)[min(EARLY)][0]
    most = max(map(len, PIECES))
    in_hbm, in_vmem = pl.BlockSpec(memory_space=pl.ANY), pl.BlockSpec(memory_space=pltpu.VMEM)
    dma = pltpu.SemaphoreType.DMA
    inner, outer, face, face_speed = pl.pallas_call(
        kernel,
        out_shape=(
            pltpu.VMEM((planes - 2, rows, depth, members), f32),
            pltpu.VMEM((2, rows, depth, members), f32),
            pltpu.VMEM((2, rows - begin, depth, members), f32),
            pltpu.VMEM((2, rows - begin, depth, members), f32),
        ),
        in_specs=[in_hbm] * 3,
        out_specs=(in_vmem,) * 4,
        scratch_shapes=[
            pltpu.VMEM((2, planes, rows + 2, depth, members), f32),
            pltpu.VMEM(shape, f32),
            pltpu.VMEM((STEPS, 2, rows, depth, members), f32),
            pltpu.VMEM((STEPS, 2, planes, rows, members), f32),
            pltpu.VMEM((STEPS, 2, planes, rows, members), f32),
            pltpu.SemaphoreType.REGULAR((2,)),
            dma((2 * len(PIECES[0]) + 5,)),
            dma((STEPS, 2, most)),
            dma((STEPS, 2, most)),
            dma((STEPS, 2)),
            dma((STEPS, 2)),
            dma((STEPS, 2)),
            dma((STEPS, 2)),
        ],
        compiler_params=pltpu.CompilerParams(
            collective_id=0, has_side_effects=True, vmem_limit_bytes=46 * 2**20
        ),
    )(field_now, earlier, speed_square)
    begun, token = pl.pallas_call(
        write_early,
        out_shape=(jax.ShapeDtypeStruct(shape, f32), pltpu.VMEM((8, 128), f32)),
        in_specs=[in_vmem] * 2,
        out_specs=(in_hbm, in_vmem),
        scratch_shapes=[dma((planes - 2 + 2 * max(EARLY),))],
        compiler_params=pltpu.CompilerParams(vmem_limit_bytes=2**20),
    )(inner, outer)
    rest = pl.pallas_call(
        functools.partial(rest_kernel, rows),
        out_shape=pltpu.VMEM((2, rows - begin, depth, members), f32),
        in_specs=[in_vmem] * 4,
        out_specs=in_vmem,
        scratch_shapes=[
            pltpu.VMEM((2, rows - begin, depth, members), f32),
            dma((2, most)),
            dma((2, most)),
        ],
        compiler_params=pltpu.CompilerParams(
            collective_id=1, has_side_effects=True, vmem_limit_bytes=8 * 2**20
        ),
    )(outer, face, face_speed, token)
    return pl.pallas_call(
        write_rest,
        out_shape=jax.ShapeDtypeStruct(shape, f32),
        in_specs=[in_vmem, in_hbm],
        out_specs=in_hbm,
        input_output_aliases={1: 0},
        scratch_shapes=[dma((2 * most,))],
        compiler_params=pltpu.CompilerParams(vmem_limit_bytes=2**20),
    )(rest, begun)


def solution(mesh):
    spec = P("lat", "lon", "lev", None)
    return jax.shard_map(local, mesh=mesh, in_specs=(spec,) * 3, out_specs=spec, check_vma=False)
```

```python
import functools

import jax
import jax.numpy as jnp
from jax import lax
from jax.experimental import pallas as pl
from jax.experimental.pallas import tpu as pltpu
from jax.sharding import PartitionSpec as P

STEPS = 4
PIECES = ((32, 32), (32, 32), (32, 32), (28, 30, 6))
EARLY = (1, 2)
MESH = pl.DeviceIdType.MESH


def cuts(step, rows):
    sizes = [size * rows // sum(PIECES[step]) for size in PIECES[step]]
    return [(sum(sizes[:index]), size) for index, size in enumerate(sizes)]


def kernel(
    now_ref, earlier_ref, speed_ref, inner_ref, outer_ref, face_ref, face_speed_ref, field, speed, halo_j, halo_k, pack_k,
    met_sem, load_sem, send_j, recv_j, send_i, recv_i, send_k, recv_k,
):
    planes, rows, depth, _ = now_ref.shape
    pieces = [cuts(step, rows) for step in range(STEPS)]
    begin = pieces[-1][min(EARLY)][0]
    place = [lax.axis_index(axis) for axis in ("lat", "lon", "lev")]
    sizes = [lax.axis_size(axis) for axis in ("lat", "lon", "lev")]
    has = [(at > 0, at < size - 1) for at, size in zip(place, sizes)]
    towards = [
        tuple({axis: at + shift} for shift in (-1, 1))
        for axis, at in zip(("lat", "lon", "lev"), place)
    ]

    lat, lon, lev = place
    x_lo, x_hi = lon // 2, lev % 2
    beside = [
        (x_lo + x_hi > 0, {"lon": lon + 2 - 4 * x_lo, "lev": lev - 1 + x_lo}),
        (x_lo + x_hi < 2, {"lon": lon + 2 - 4 * x_lo, "lev": lev + x_lo}),
        (lev >= 2, {"lev": lev - 2}),
        (lev < sizes[2] - 2, {"lev": lev + 2}),
        (lon >= 0, {"lon": lon + 1 - 2 * (lon % 2)}),
    ]

    def greet(semaphore, devices):
        count = 0
        for there, device in devices:
            count = count + there.astype(jnp.int32)

            @pl.when(there)
            def _():
                pl.semaphore_signal(semaphore, inc=1, device_id=device, device_id_type=MESH)

        return count

    barrier = pltpu.get_barrier_semaphore()
    count = greet(barrier, beside + [(has[0][side], towards[0][side]) for side in range(2)])

    faces = 2 * len(pieces[0])
    spans = [(plane, 1, at, size) for at, size in pieces[0] for plane in (0, planes - 1)]
    spans.append((1, planes - 2, 0, rows))
    loads = [
        pltpu.make_async_copy(
            now_ref.at[pl.ds(plane, count), pl.ds(at, size)],
            field.at[0, pl.ds(plane, count), pl.ds(at + 1, size)],
            load_sem.at[index],
        )
        for index, (plane, count, at, size) in enumerate(spans)
    ]
    loads.append(pltpu.make_async_copy(earlier_ref, field.at[1, :, pl.ds(1, rows)], load_sem.at[faces + 1]))
    loads.append(pltpu.make_async_copy(speed_ref, speed, load_sem.at[faces + 2]))
    loads += [
        pltpu.make_async_copy(
            speed_ref.at[(planes - 1) * side, pl.ds(begin, rows - begin)], face_speed_ref.at[side], load_sem.at[faces + 3 + side]
        )
        for side in range(2)
    ]
    for load in loads[:faces]:
        load.start()

    pl.semaphore_wait(barrier, count)

    def copy_j(step, piece, side):
        at, size = pieces[step][piece]
        if step == STEPS - 1 and at >= begin:
            source = face_ref.at[side, pl.ds(at - begin, size)]
        else:
            source = field.at[step % 2, (planes - 1) * side, pl.ds(at + 1, size)]
        return pltpu.make_async_remote_copy(
            src_ref=source,
            dst_ref=halo_j.at[step, 1 - side, pl.ds(at, size)],
            send_sem=send_j.at[step, side, piece],
            recv_sem=recv_j.at[step, 1 - side, piece],
            device_id=towards[0][side],
            device_id_type=MESH,
        )

    def copy_i(step, side):
        return pltpu.make_async_remote_copy(
            src_ref=field.at[step % 2, :, 1 + (rows - 1) * side],
            dst_ref=field.at[step % 2, :, (rows + 1) * (1 - side)],
            send_sem=send_i.at[step, side],
            recv_sem=recv_i.at[step, 1 - side],
            device_id=towards[1][side],
            device_id_type=MESH,
        )

    def copy_k(step, side):
        return pltpu.make_async_remote_copy(
            src_ref=pack_k.at[step, side],
            dst_ref=halo_k.at[step, 1 - side],
            send_sem=send_k.at[step, side],
            recv_sem=recv_k.at[step, 1 - side],
            device_id=towards[2][side],
            device_id_type=MESH,
        )

    def pack(step):
        def row(i, _):
            for plane in range(planes):
                for side in range(2):
                    pack_k[step, side, plane, pl.ds(i, 1), :] = field[step % 2, plane, i + 1, pl.ds((depth - 1) * side, 1), :]
            return 0

        lax.fori_loop(0, rows, row, 0)

    def send_sides(step):
        for side in range(2):
            @pl.when(has[1][side])
            def _():
                copy_i(step, side).start()

        for side in range(2):
            @pl.when(has[2][side])
            def _():
                copy_k(step, side).start()

    def wait_sides(step):
        for side in range(2):
            @pl.when(has[1][1 - side])
            def _():
                copy_i(step, side).wait_recv()

            @pl.when(has[2][1 - side])
            def _():
                copy_k(step, side).wait_recv()

    def wait_sides_sent(step):
        for side in range(2):
            @pl.when(has[1][side])
            def _():
                copy_i(step, side).wait_send()

            @pl.when(has[2][side])
            def _():
                copy_k(step, side).wait_send()

    def send_piece(step, piece):
        for side in range(2):
            @pl.when(has[0][side])
            def _():
                copy_j(step, piece, side).start()

    def wait_piece_sent(step, piece):
        for side in range(2):
            @pl.when(has[0][side])
            def _():
                copy_j(step, piece, side).wait_send()

    def wait_piece(step, piece):
        for side in range(2):
            @pl.when(has[0][1 - side])
            def _():
                copy_j(step, piece, side).wait_recv()

    def each(count, body):
        def one(index, _):
            body(index)
            return 0

        if count:
            lax.fori_loop(0, count, one, 0)

    for piece in range(len(pieces[0])):
        loads[2 * piece].wait()
        loads[2 * piece + 1].wait()
        send_piece(0, piece)

    for load in loads[faces:]:
        load.start()

    for index in range(2):
        pl.semaphore_wait(met_sem.at[index], greet(met_sem.at[index], beside))

    for side in range(2):
        @pl.when(jnp.logical_not(has[1][side]))
        def _():
            for slot in range(2):
                field[slot, :, (rows + 1) * side] = jnp.zeros((planes, depth, 128), jnp.float32)

        @pl.when(jnp.logical_not(has[2][side]))
        def _():
            for step in range(STEPS):
                for plane in range(planes):
                    halo_k[step, side, plane] = jnp.zeros((rows, 128), jnp.float32)

        @pl.when(jnp.logical_not(has[0][side]))
        def _():
            def row(i, _):
                halo_j[0, side, i] = jnp.zeros((depth, 128), jnp.float32)
                return 0

            lax.fori_loop(0, rows, row, 0)

    loads[faces].wait()
    pack(0)
    send_sides(0)
    for load in loads[faces + 1:]:
        load.wait()

    level = lax.broadcasted_iota(jnp.int32, (depth, 128), 0)
    first, last = level == 0, level == depth - 1

    def compute_row(step, i, to_face=False):
        old, new = step % 2, (step + 1) % 2
        slots = [jnp.where(has[0][side], step, 0) for side in range(2)]
        for plane in range(planes):
            here = field[old, plane, i + 1]
            terms = []
            if plane > 0:
                terms.append(field[old, plane - 1, i + 1])
            elif step < STEPS - 1:
                terms.append(halo_j[slots[0], 0, i])
            if plane < planes - 1:
                terms.append(field[old, plane + 1, i + 1])
            elif step < STEPS - 1:
                terms.append(halo_j[slots[1], 1, i])
            terms += [field[old, plane, i], field[old, plane, i + 2]]
            terms.append(jnp.where(first, halo_k[step, 0, plane, pl.ds(i, 1), :], pltpu.roll(here, 1, 0)))
            terms.append(jnp.where(last, halo_k[step, 1, plane, pl.ds(i, 1), :], pltpu.roll(here, depth - 1, 0)))
            spread = functools.reduce(jnp.add, terms) - 6.0 * here
            later = 2.0 * here - field[new, plane, i + 1] + speed[plane, i] * spread
            if step < STEPS - 1:
                field[new, plane, i + 1] = later
                if to_face and plane in (0, planes - 1):
                    face_ref[plane // (planes - 1), i - begin] = later
            elif plane in (0, planes - 1):
                outer_ref[plane // (planes - 1), i] = later
            else:
                inner_ref[plane - 1, i] = later

    def add_halo(step, i):
        for side in range(2):
            plane = (planes - 1) * side
            slot = jnp.where(has[0][side], step, 0)
            outer_ref[side, i] = outer_ref[side, i] + speed[plane, i] * halo_j[slot, side, i]

    for step in range(STEPS - 1):
        wait_sides(step)
        if step > 0:
            wait_sides_sent(step - 1)
        sent = free = 0
        for piece, (at, size) in enumerate(pieces[step]):
            while step > 0 and free < len(pieces[step - 1]) and pieces[step - 1][free][0] < at + size:
                wait_piece_sent(step - 1, free)
                free += 1
            wait_piece(step, piece)
            kept = min(max(begin - at, 0), size) if step == STEPS - 2 else size
            each(kept, lambda i: compute_row(step, at + i))
            each(size - kept, lambda i: compute_row(step, at + kept + i, True))
            while sent < len(pieces[step + 1]) and sum(pieces[step + 1][sent]) <= at + size:
                if step + 1 < STEPS - 1:
                    send_piece(step + 1, sent)
                else:
                    @pl.when(is_early(place[1], sent))
                    def _():
                        send_piece(step + 1, sent)

                sent += 1
        pack(step + 1)
        send_sides(step + 1)

    step = STEPS - 1
    wait_sides(step)
    each(rows, lambda i: compute_row(step, i))
    for piece in range(len(pieces[step - 1])):
        wait_piece_sent(step - 1, piece)
    for before in (step - 1, step):
        wait_sides_sent(before)
    for piece, (at, size) in enumerate(pieces[step]):
        @pl.when(is_early(place[1], piece))
        def _():
            wait_piece(step, piece)
            each(size, lambda i: add_halo(step, at + i))
            wait_piece_sent(step, piece)


def is_early(lon, piece):
    return jnp.where(lon % 2 == 0, EARLY[0], EARLY[1]) > piece


def rest_kernel(rows, outer_ref, face_ref, face_speed_ref, token_ref, rest_ref, halo, send, recv):
    del token_ref
    depth = face_ref.shape[2]
    pieces = cuts(STEPS - 1, rows)
    begin = pieces[min(EARLY)][0]
    at_lat, at_lon = lax.axis_index("lat"), lax.axis_index("lon")
    has = (at_lat > 0, at_lat < lax.axis_size("lat") - 1)
    towards = ({"lat": at_lat - 1}, {"lat": at_lat + 1})

    barrier = pltpu.get_barrier_semaphore()
    for side in range(2):
        @pl.when(has[side])
        def _():
            pl.semaphore_signal(barrier, inc=1, device_id=towards[side], device_id_type=MESH)

    @pl.when(at_lon % 2 == 1)
    def _():
        pl.delay(2000)

    pl.semaphore_wait(barrier, has[0].astype(jnp.int32) + has[1].astype(jnp.int32))

    def copy(piece, side):
        at, size = pieces[piece]
        return pltpu.make_async_remote_copy(
            src_ref=face_ref.at[side, pl.ds(at - begin, size)],
            dst_ref=halo.at[1 - side, pl.ds(at - begin, size)],
            send_sem=send.at[side, piece],
            recv_sem=recv.at[1 - side, piece],
            device_id=towards[side],
            device_id_type=MESH,
        )

    late = range(min(EARLY), len(pieces))
    for piece in late:
        for side in range(2):
            @pl.when(has[side] & jnp.logical_not(is_early(at_lon, piece)))
            def _():
                copy(piece, side).start()

    for side in range(2):
        @pl.when(jnp.logical_not(has[side]))
        def _():
            def row(i, _):
                halo[side, i] = jnp.zeros((depth, 128), jnp.float32)
                return 0

            lax.fori_loop(0, rows - begin, row, 0)

    for piece in late:
        at, size = pieces[piece]

        @pl.when(jnp.logical_not(is_early(at_lon, piece)))
        def _():
            for side in range(2):
                @pl.when(has[1 - side])
                def _():
                    copy(piece, side).wait_recv()

            def row(i, _):
                for side in range(2):
                    on = at - begin + i
                    rest_ref[side, on] = outer_ref[side, at + i] + face_speed_ref[side, on] * halo[side, on]
                return 0

            lax.fori_loop(0, size, row, 0)

    for piece in late:
        for side in range(2):
            @pl.when(has[side] & jnp.logical_not(is_early(at_lon, piece)))
            def _():
                copy(piece, side).wait_send()


def run(copies):
    for condition, copy in copies:
        @pl.when(condition)
        def _():
            copy.start()

    for condition, copy in copies:
        @pl.when(condition)
        def _():
            copy.wait()


def write_early(inner_ref, outer_ref, out_ref, token_ref, sem):
    planes, rows = out_ref.shape[:2]
    lon = lax.axis_index("lon")
    copies = [
        (lon >= 0, pltpu.make_async_copy(inner_ref.at[plane], out_ref.at[plane + 1], sem.at[plane]))
        for plane in range(planes - 2)
    ]
    for piece, (at, size) in enumerate(cuts(STEPS - 1, rows)[:max(EARLY)]):
        for side in range(2):
            copies.append((is_early(lon, piece), pltpu.make_async_copy(
                outer_ref.at[side, pl.ds(at, size)],
                out_ref.at[(planes - 1) * side, pl.ds(at, size)],
                sem.at[len(copies)],
            )))
    run(copies)
    token_ref[...] = jnp.zeros_like(token_ref)


def write_rest(rest_ref, begun_ref, out_ref, sem):
    del begun_ref
    planes, rows = out_ref.shape[:2]
    lon = lax.axis_index("lon")
    pieces = cuts(STEPS - 1, rows)
    begin = pieces[min(EARLY)][0]
    spans = [
        (side, at, size, jnp.logical_not(is_early(lon, piece)))
        for piece, (at, size) in enumerate(pieces) if piece >= min(EARLY) for side in range(2)
    ]
    run([
        (condition, pltpu.make_async_copy(
            rest_ref.at[side, pl.ds(at - begin, size)],
            out_ref.at[(planes - 1) * side, pl.ds(at, size)],
            sem.at[index]))
        for index, (side, at, size, condition) in enumerate(spans)
    ])


def local(field_now, earlier, speed_square):
    planes, rows, depth, members = field_now.shape
    shape, f32 = field_now.shape, jnp.float32
    begin = cuts(STEPS - 1, rows)[min(EARLY)][0]
    most = max(map(len, PIECES))
    in_hbm, in_vmem = pl.BlockSpec(memory_space=pl.ANY), pl.BlockSpec(memory_space=pltpu.VMEM)
    dma = pltpu.SemaphoreType.DMA
    inner, outer, face, face_speed = pl.pallas_call(
        kernel,
        out_shape=(
            pltpu.VMEM((planes - 2, rows, depth, members), f32),
            pltpu.VMEM((2, rows, depth, members), f32),
            pltpu.VMEM((2, rows - begin, depth, members), f32),
            pltpu.VMEM((2, rows - begin, depth, members), f32),
        ),
        in_specs=[in_hbm] * 3,
        out_specs=(in_vmem,) * 4,
        scratch_shapes=[
            pltpu.VMEM((2, planes, rows + 2, depth, members), f32),
            pltpu.VMEM(shape, f32),
            pltpu.VMEM((STEPS, 2, rows, depth, members), f32),
            pltpu.VMEM((STEPS, 2, planes, rows, members), f32),
            pltpu.VMEM((STEPS, 2, planes, rows, members), f32),
            pltpu.SemaphoreType.REGULAR((2,)),
            dma((2 * len(PIECES[0]) + 5,)),
            dma((STEPS, 2, most)),
            dma((STEPS, 2, most)),
            dma((STEPS, 2)),
            dma((STEPS, 2)),
            dma((STEPS, 2)),
            dma((STEPS, 2)),
        ],
        compiler_params=pltpu.CompilerParams(
            collective_id=0, has_side_effects=True, vmem_limit_bytes=46 * 2**20
        ),
    )(field_now, earlier, speed_square)
    begun, token = pl.pallas_call(
        write_early,
        out_shape=(jax.ShapeDtypeStruct(shape, f32), pltpu.VMEM((8, 128), f32)),
        in_specs=[in_vmem] * 2,
        out_specs=(in_hbm, in_vmem),
        scratch_shapes=[dma((planes - 2 + 2 * max(EARLY),))],
        compiler_params=pltpu.CompilerParams(vmem_limit_bytes=2**20),
    )(inner, outer)
    rest = pl.pallas_call(
        functools.partial(rest_kernel, rows),
        out_shape=pltpu.VMEM((2, rows - begin, depth, members), f32),
        in_specs=[in_vmem] * 4,
        out_specs=in_vmem,
        scratch_shapes=[
            pltpu.VMEM((2, rows - begin, depth, members), f32),
            dma((2, most)),
            dma((2, most)),
        ],
        compiler_params=pltpu.CompilerParams(
            collective_id=1, has_side_effects=True, vmem_limit_bytes=8 * 2**20
        ),
    )(outer, face, face_speed, token)
    return pl.pallas_call(
        write_rest,
        out_shape=jax.ShapeDtypeStruct(shape, f32),
        in_specs=[in_vmem, in_hbm],
        out_specs=in_hbm,
        input_output_aliases={1: 0},
        scratch_shapes=[dma((2 * most,))],
        compiler_params=pltpu.CompilerParams(vmem_limit_bytes=2**20),
    )(rest, begun)


def solution(mesh):
    spec = P("lat", "lon", "lev", None)
    return jax.shard_map(local, mesh=mesh, in_specs=(spec,) * 3, out_specs=spec, check_vma=False)
```
